128 devices in a mesh: dom: 8 (over y, x_hi), band: 8 (over z, core), sub: 2 (over x_lo).
Axes of the slice: x: 4 (x_hi: 2, x_lo: 2; x = x_hi * 2 + x_lo), y: 4, z: 4, core: 2. Of those that a mesh axis runs over, the one named last changes fastest.
Arguments:
- orbitals: float32 [8, 64, 64, 4096], P('dom', 'band', 'sub'), may hold values from -6 to 6
- occupations: float32 [8, 64], P('dom', 'band'), may hold values from 0.0003 to 0.003
- ext_potential: float32 [8, 64, 4096], P('dom', 'sub'), may hold values from 0 to 4
- core_range: int32 [8, 2], P('dom'), may hold values from 0 to 16, as said below
Outputs:
- orbitals_out: float32 [8, 64, 64, 4096], P('dom', 'band', 'sub')
- domain_potential: float32 [8, 64, 4096], P('dom', 'sub')
The draws below stay inside these ranges and needn't reach their ends.
Inputs may be any that keep to these rules, and one draw needn't show every extreme that they name: core_range[d, 0] is 0 or 1 and core_range[d, 1] is 15 or 16.
All inputs are finite; a program needn't handle non-finite values.
Results may differ from the reference program's by a relative error of at most 0.00025.
Values sent between devices are 32-bit elements; how exact they have to be, the bound alone decides.
A program may use at most 128 MiB of HBM per device.

```python
import math
import jax
import jax.numpy as jnp
from jax import lax

EDGE = 64
MARGIN = 8
BLOCK = 4
ORBITALS = 64
STEPS = 3
CORE = 48
DOMS = 8
GX = 384
N_DOM = 8


def draw_core_range(key, part):
    first_key = jax.random.fold_in(key, 11)
    second_key = jax.random.fold_in(key, 12)
    starts = jax.random.randint(first_key, (DOMS, 1), 0, 2)
    finish = jax.random.randint(second_key, (DOMS, 1), EDGE // BLOCK - 1, EDGE // BLOCK + 1)
    return jnp.concatenate([starts, finish], axis=1).astype(jnp.int32)


def draw_orbitals(key, part):
    base_key = jax.random.fold_in(key, 21)
    domain_key = jax.random.fold_in(key, 22)
    depth_key = jax.random.fold_in(key, 23)
    length_key = jax.random.fold_in(key, 24)
    groups = 8
    group_cells = EDGE // groups
    shape = (DOMS, ORBITALS, EDGE, EDGE, EDGE)
    spread = 0.5
    base = jax.random.normal(base_key, shape, jnp.float32)
    domain_factor = jnp.exp(jax.random.uniform(domain_key, (DOMS,), jnp.float32, -spread, spread))
    depth_factor = jnp.exp(jax.random.uniform(depth_key, (groups,), jnp.float32, -spread, spread))
    depth_factor = jnp.repeat(depth_factor, group_cells)
    length_factor = jnp.exp(jax.random.uniform(length_key, (DOMS, groups), jnp.float32, -spread, spread))
    length_factor = jnp.repeat(length_factor, group_cells, axis=1)
    amplitude = domain_factor[:, None, None] * depth_factor[None, :, None] * length_factor[:, None, :]
    values = jnp.clip(base * amplitude[:, None, :, :, None], -6.0, 6.0)
    return values.reshape(DOMS, ORBITALS, EDGE, EDGE * EDGE).astype(jnp.float32)


def block_scale(key, dims, pieces, low, top_value):
    def one(dim, blocks):
        steps = jax.random.uniform(jax.random.fold_in(jax.random.fold_in(key, 6), dim), (blocks,), jnp.float32, low / len(pieces), top_value / len(pieces))
        return jnp.repeat(jnp.exp(steps), dims[dim] // blocks).reshape((-1,) + (1,) * (len(dims) - dim - 1))

    level = one(*pieces[0])
    for cut in pieces[1:]:
        level = level * one(*cut)
    return level


def setup_inputs(seed: int = 0) -> dict:
    streams_of = jax.random.split(jax.random.key(seed), 5)
    orbitals = draw_orbitals(jax.random.fold_in(streams_of[4], 71), 0)
    occupations = jnp.clip(jnp.exp(math.log(0.003) - 2.3025851 * jax.random.uniform(streams_of[1], (DOMS, ORBITALS), jnp.float32) ** block_scale(streams_of[1], (DOMS, ORBITALS), ((0, 8), (1, 8)), -0.2, 0.2)), 0.0003, 0.003)
    ext_potential = jnp.clip(4.0 * jax.random.uniform(streams_of[2], (DOMS, EDGE, EDGE * EDGE), jnp.float32) ** block_scale(streams_of[2], (DOMS, EDGE, EDGE * EDGE), ((0, 8), (1, 2)), -0.2, 0.2), 0.0, 4.0)
    core_range = draw_core_range(jax.random.fold_in(streams_of[4], 71), 0)
    return {"orbitals": orbitals, "occupations": occupations, "ext_potential": ext_potential, "core_range": core_range}


time_step = 0.2
screen = 0.02
eps = 1e-06
highest = lax.Precision.HIGHEST

def cas_table(row_ids, col_ids, length):
    product = row_ids[:, None] * col_ids[None, :] % length
    angle = 2.0 * jnp.pi / length * product.astype(jnp.float32)
    return jnp.cos(angle) + jnp.sin(angle)

def eigen_values(wave_ids, length):
    return 2.0 - 2.0 * jnp.cos(2.0 * jnp.pi / length * wave_ids.astype(jnp.float32))

def transform(values, along):
    length = values.shape[along]
    ids_all = jnp.arange(length, dtype=jnp.int32)
    kernel = cas_table(ids_all, ids_all, length)
    shifted = jnp.moveaxis(values, along, -1)
    result = jnp.dot(shifted, kernel, precision=highest)
    return jnp.moveaxis(result, -1, along)

def laplace(orbitals):
    along_z = jnp.roll(orbitals, 1, 2) + jnp.roll(orbitals, -1, 2)
    along_y = jnp.roll(orbitals, 1, 4) + jnp.roll(orbitals, -1, 4)
    padded = jnp.pad(orbitals, ((0, 0), (0, 0), (0, 0), (1, 1), (0, 0)))
    along_x = padded[:, :, :, 2:] + padded[:, :, :, :-2]
    return along_z + along_x + along_y - 6.0 * orbitals

def hartree(density_grid):
    spectrum = transform(transform(transform(density_grid, 0), 1), 2)
    edge_ids = jnp.arange(EDGE, dtype=jnp.int32)
    length_ids = jnp.arange(GX, dtype=jnp.int32)
    green = 1.0 / (eigen_values(edge_ids, EDGE)[:, None, None] + eigen_values(length_ids, GX)[None, :, None] + eigen_values(edge_ids, EDGE)[None, None, :] + screen)
    potential = transform(transform(transform(spectrum * green, 0), 1), 2)
    return potential / (GX * EDGE * EDGE)

def reference(orbitals, occupations, ext_potential, core_range):
    orbitals = orbitals.reshape(DOMS, ORBITALS, EDGE, EDGE, EDGE)
    ext_potential = ext_potential.reshape(DOMS, EDGE, EDGE, EDGE)
    cell_ids = jnp.arange(EDGE, dtype=jnp.int32)
    core_mask = ((cell_ids[None, :] >= core_range[:, 0:1] * BLOCK) & (cell_ids[None, :] < core_range[:, 1:2] * BLOCK)).astype(jnp.float32)
    cell_count = float(EDGE ** 3)
    potential_window = jnp.zeros_like(ext_potential)
    for repeat in range(STEPS):
        density = jnp.einsum('do,dozxy->dzxy', occupations, orbitals * orbitals, precision=highest)
        density = density * core_mask[:, None, :, None]
        own_core = density[:, :, MARGIN:MARGIN + CORE]
        from_right = jnp.roll(density[:, :, :MARGIN], -1, 0)
        from_left = jnp.roll(density[:, :, EDGE - MARGIN:], 1, 0)
        density_grid = own_core + jnp.pad(from_left, ((0, 0), (0, 0), (0, CORE - MARGIN), (0, 0))) + jnp.pad(from_right, ((0, 0), (0, 0), (CORE - MARGIN, 0), (0, 0)))
        density_grid = density_grid.transpose(1, 0, 2, 3).reshape(EDGE, GX, EDGE)
        potential = hartree(density_grid).reshape(EDGE, N_DOM, CORE, EDGE).transpose(1, 0, 2, 3)
        potential_window = jnp.concatenate([jnp.roll(potential, 1, 0)[:, :, CORE - MARGIN:], potential, jnp.roll(potential, -1, 0)[:, :, :MARGIN]], axis=2)
        half_step = jnp.exp(-0.5 * time_step * (potential_window + ext_potential))[:, None]
        scaled = orbitals * half_step
        stepped = (scaled + 0.5 * time_step * laplace(scaled)) * half_step
        squares = lax.optimization_barrier(jnp.sum(stepped * stepped, axis=(2, 3, 4)))
        orbitals = stepped / jnp.sqrt(squares / cell_count + eps)[:, :, None, None, None]
    return (orbitals.reshape(DOMS, ORBITALS, EDGE, EDGE * EDGE), potential_window.reshape(DOMS, EDGE, EDGE * EDGE))
```

```python
import functools

import jax
import jax.numpy as jnp
import numpy as np
from jax import lax
from jax.experimental import pallas as pl
from jax.experimental.pallas import tpu as pltpu
from jax.sharding import PartitionSpec as P

EDGE = 64
MARGIN = 8
BLOCK = 4
STEPS = 3
CORE = 48
GX = 384
N_DOM = 8
N_BAND = 8
TIME = 0.2
SCREEN = 0.02
EPS = 1e-06
CELLS = float(EDGE**3)
F32 = jnp.float32
HIGH = lax.Precision.HIGH
MESH = pl.DeviceIdType.MESH


def cas(rows, cols, n):
    angle = 2.0 * np.pi / n * ((rows[:, None] * cols[None, :]) % n)
    return np.cos(angle) + np.sin(angle)


def tables():
    ids = np.arange(EDGE)
    full = cas(ids, ids, EDGE)
    w_y = np.kron(np.eye(2), full)
    w_h = np.concatenate([np.concatenate([full, full], 1), np.zeros((64, 128))], 0)
    w_z = np.kron(np.eye(4), np.concatenate([full[:32], full[:32]], 1))
    both = np.concatenate([full, full], 0)
    halo0 = np.tile(both[:, [63, 32]], (1, 16))
    halo1 = np.tile(both[:, [31, 0]], (1, 16))
    w_i = np.concatenate(
        [np.kron(np.eye(4), b) for b in (both[:, :32], both[:, 32:], halo0, halo1)], 1
    )
    lam = 2.0 - 2.0 * np.cos(2.0 * np.pi / EDGE * ids)
    a = lam[:, None] + lam[None, :] + SCREEN
    r = 1.0 / (1.0 + a / 2 + np.sqrt(a + a * a / 4))
    scale = 1.0 / (1.0 / r - r) / (EDGE * EDGE)
    sign = np.where(ids % 2 == 1, -1.0, 1.0)[None, :]
    rows = [r, scale, scale * sign]
    for k in range(2, 10):
        rows.append(r ** (CORE * k - 63) / (1.0 - r**GX))
    modes = np.stack(rows)
    modes = np.concatenate([modes, modes], 2).reshape(11, N_BAND, 8, 128).transpose(1, 0, 2, 3)
    return [np.asarray(v, np.float32) for v in (w_y, w_h, w_z, w_i, modes)]


def dot(a, b, dims=((1,), (0,))):
    return lax.dot_general(a, b, (dims, ((), ())), precision=HIGH, preferred_element_type=F32)


def kernel(
    orb_hbm, occ, ext_hbm, core, wy_hbm, wh_hbm, wz_hbm, wi_hbm, modes_hbm,
    out_hbm, pot_hbm, inv_out,
    U, HALF, EXT, VB, WY, WH, WZ, WI, MODES, OCC8, W8, INV,
    SB, RA, S1, RB, S2, PP, PW, FS, FR, MV, QB, OB, R4, AG, EDGES, ER, EXTE, EXTR, HH, SH, NBO, NB, NR,
    l_u, l_c, ssA, rsA, ssB, rsB, ssF, rsF, ssM, rsM, ss4, rs4, ssG, rsG, ssH, rsH, ssE, rsE,
    ssX, rsX, ssN, rsN, l_o,
):
    d = lax.axis_index("dom")
    b = lax.axis_index("band")
    h = lax.axis_index("sub")
    zi = b // 2
    co = b % 2
    mate = zi * 2 + (1 - co)
    other = 1 - h

    def zpeer(k):
        return ((zi + k) % 4) * 2 + co

    loads = [pltpu.make_async_copy(orb_hbm.at[0, o], U.at[o], l_u.at[o]) for o in range(8)]
    loads += [
        pltpu.make_async_copy(src, dst, l_c.at[i])
        for i, (src, dst) in enumerate(
            (
                (ext_hbm.at[0], EXT),
                (wy_hbm, WY),
                (wh_hbm, WH),
                (wz_hbm, WZ),
                (wi_hbm, WI),
                (modes_hbm.at[b], MODES),
            )
        )
    ]
    for c in loads:
        c.start()

    barrier = pltpu.get_barrier_semaphore()

    def greet(dev):
        pl.semaphore_signal(barrier, inc=1, device_id=dev, device_id_type=MESH)

    greet({"band": mate})
    for k in range(1, 4):
        greet({"band": zpeer(k)})
    greet({"sub": other})
    for k in range(1, 8):
        greet({"dom": (d + k) % 8})

    def send(src, dst, ss, rs, dev):
        return pltpu.make_async_remote_copy(
            src_ref=src, dst_ref=dst, send_sem=ss, recv_sem=rs, device_id=dev, device_id_type=MESH
        )

    lane = lax.broadcasted_iota(jnp.int32, (8, 128), 1)
    low = lane < 64
    lane16 = lax.broadcasted_iota(jnp.int32, (16, 128), 1)
    lane32 = lax.broadcasted_iota(jnp.int32, (32, 128), 1)
    row32 = lax.broadcasted_iota(jnp.int32, (32, 128), 0)
    low32 = lane32 < 64
    first_y = (lane32 == 0) | (lane32 == 64)
    last_y = (lane32 == 63) | (lane32 == 127)
    slot = (lane % 32) // 2
    zero8 = jnp.zeros((8, 128), F32)

    for o in range(8):
        OCC8[o : o + 1, :] = jnp.full((1, 128), occ[0, o], F32)
    W8[...] = OCC8[...]
    INV[...] = jnp.ones((8, 8, 128), F32)

    for c in loads:
        c.wait()

    r = MODES[0]
    power = jnp.ones((8, 128), F32)
    for i in range(64):
        PW[i] = power
        power = power * r

    def lanes(tile):
        return pl.ds(tile * 128, 128)

    for tile in range(32):
        EXTE[0, tile : tile + 1, :] = EXT[31:32, lanes(tile)]
        EXTE[1, tile : tile + 1, :] = EXT[0:1, lanes(tile)]

    def first_edges(o, carry):
        for tile in range(32):
            EDGES[0, 0, o, tile : tile + 1, :] = U[o, 31:32, lanes(tile)]
            EDGES[0, 1, o, tile : tile + 1, :] = U[o, 0:1, lanes(tile)]
        return carry

    lax.fori_loop(0, 8, first_edges, 0)

    pl.semaphore_wait(barrier, 12)

    ext_copy = send(EXTE, EXTR, ssX.at[0], rsX.at[0], {"sub": other})
    ext_copy.start()

    low_x = core[0, 0] * BLOCK
    high_x = core[0, 1] * BLOCK

    def step(st, carry):
        edge_copy = send(EDGES.at[st], ER.at[st], ssE.at[st], rsE.at[st], {"sub": other})
        edge_copy.start()

        for g in range(8):
            tiles = []
            for t in range(4):
                tile = 4 * g + t
                acc = jnp.zeros((32, 128), F32)
                for o in range(8):
                    value = U[o, :, lanes(tile)]
                    acc = acc + value * value * W8[o : o + 1, :]
                x = 2 * tile + lane32 // 64
                tiles.append(jnp.where((x >= low_x) & (x < high_x), acc, 0.0))
            rho = jnp.concatenate(tiles, 0)
            out = dot(WY[...], rho, ((1,), (1,)))
            for x2 in range(2):
                for c in range(2):
                    for z in range(4):
                        row = x2 * 64 + (2 * z + c) * 8
                        SB[c, z, 2 * g + x2] = out[row : row + 8]

        copy_a = send(SB.at[1 - co], RA.at[st], ssA.at[st], rsA.at[st], {"band": mate})
        copy_a.start()
        copy_a.wait_recv()
        copies_b = []
        for k in range(1, 4):
            z = (zi + k) % 4
            S1[k] = SB[co, z] + RA[st, z]
            copy = send(
                S1.at[k], RB.at[st, k - 1], ssB.at[st, k - 1], rsB.at[st, k - 1], {"band": zpeer(k)}
            )
            copy.start()
            copies_b.append(copy)
        S1[0] = SB[co, zi] + RA[st, zi]
        for copy in copies_b:
            copy.wait_recv()
        total = S1[0] + RB[st, 0] + RB[st, 1] + RB[st, 2]

        out = dot(total.reshape(128, 128), WZ[...])
        scale = MODES[1 + h]
        r = MODES[0]
        for g in range(8):
            for t in range(4):
                for x2 in range(2):
                    row = (2 * g + x2) * 8
                    S2[8 * g + 2 * t + x2] = out[row : row + 8, t * 128 : t * 128 + 128] * scale

        p = zero8
        for i in range(64):
            p = p * r + jnp.where(low, S2[i], S2[63 - i])
            PP[i] = p
        MV[st, d] = p
        moment_copies = []
        for k in range(1, 8):
            copy = send(
                MV.at[st, d], MV.at[st, d], ssM.at[st, k - 1], rsM.at[st, k - 1], {"dom": (d + k) % 8}
            )
            copy.start()
            moment_copies.append(copy)

        def response(x):
            return jnp.where(low, PP[x] - S2[x], PP[63 - x])

        side_copies = []
        for side, base, peer in ((0, 48, (d + 1) % 8), (1, 0, (d + 7) % 8)):
            for m in range(8):
                even = response(base + 2 * m)
                odd = response(base + 2 * m + 1)
                even = even + pltpu.roll(even, 64, 1)
                odd = odd + pltpu.roll(odd, 64, 1)
                FS[side, m] = jnp.where(low, even, odd)
            copy = send(
                FS.at[side], FR.at[st, side], ssF.at[st, side], rsF.at[st, side], {"dom": peer}
            )
            copy.start()
            side_copies.append(copy)

        for copy in moment_copies:
            copy.wait_recv()
        for copy in side_copies:
            copy.wait_recv()

        incoming = zero8
        for k in range(2, 10):
            moved = jnp.where(low, MV[st, (d + 16 - k) % 8], MV[st, (d + k) % 8])
            incoming = incoming + MODES[1 + k] * moved
        near = jnp.where(low, MV[st, (d + 7) % 8], MV[st, (d + 1) % 8])
        for i in range(64):
            value = PP[i] + PW[i] * incoming
            if i >= 16:
                value = value + PW[i - 15] * near
            PP[i] = value
        for x in range(64):
            value = response(x)
            if x < 16:
                part = FR[st, 0, x // 2]
                value = value + jnp.where(low if x % 2 == 0 else ~low, part, 0.0)
            if x >= 48:
                part = FR[st, 1, (x - 48) // 2]
                value = value + jnp.where(low if x % 2 == 0 else ~low, part, 0.0)
            g, t, x2 = x // 8, (x % 8) // 2, x % 2
            row = (2 * g + x2) * 8
            QB[row : row + 8, t * 128 : t * 128 + 128] = value

        out = dot(QB[...], WI[...])
        for q in range(2):
            halo = zero8
            for g in range(8):
                for x2 in range(2):
                    j = 2 * g + x2
                    OB[q, j] = out[j * 8 : j * 8 + 8, q * 128 : q * 128 + 128]
                    part = out[j * 8 : j * 8 + 8, (2 + q) * 128 : (2 + q) * 128 + 128]
                    halo = jnp.where(slot == x2 * 8 + g, part, halo)
            OB[q, 16] = halo
        copy_4 = send(OB.at[other], R4.at[st], ss4.at[st], rs4.at[st], {"sub": other})
        copy_4.start()
        copy_4.wait_recv()
        AG[st, b] = OB[h] + R4[st]

        gather = []
        for k in range(1, 4):
            copy = send(
                AG.at[st, b], AG.at[st, b], ssG.at[st, k - 1], rsG.at[st, k - 1], {"band": zpeer(k)}
            )
            copy.start()
            gather.append(copy)
        forward = [send(AG.at[st, b], AG.at[st, b], ssH.at[st, 0], rsH.at[st, 0], {"band": mate})]
        forward[0].start()
        for k in range(1, 4):
            gather[k - 1].wait_recv()
            came = zpeer(4 - k)
            copy = send(
                AG.at[st, came], AG.at[st, came], ssH.at[st, k], rsH.at[st, k], {"band": mate}
            )
            copy.start()
            forward.append(copy)
        for copy in forward:
            copy.wait_recv()

        for g in range(8):
            parts = [AG[st, :, 2 * g + x2].reshape(64, 128) for x2 in range(2)]
            cols = jnp.concatenate(parts, 0).T
            out = dot(cols, WY[...])
            for t in range(4):
                tile = 4 * g + t
                value = out[t * 32 : t * 32 + 32]
                VB[:, lanes(tile)] = value
                HALF[:, lanes(tile)] = jnp.exp(-0.5 * TIME * (value + EXT[:, lanes(tile)]))

        @pl.when(st == 0)
        def _():
            ext_copy.wait()

        edge_copy.wait_recv()
        rims = AG[st, :, 16].reshape(64, 128)
        out = dot(jnp.concatenate([rims, rims], 0).T, WH[...])
        low16 = lane16 < 64
        for t in range(4):
            value = jnp.where(low16, out[t * 32 : t * 32 + 16], out[t * 32 + 16 : t * 32 + 32])
            for g in range(8):
                tile = 4 * g + t
                for q in range(2):
                    HH[q, tile : tile + 1, :] = value[2 * g + q : 2 * g + q + 1]
        for q in range(2):
            half = jnp.exp(-0.5 * TIME * (HH[q] + EXTR[q]))
            for o in range(8):
                SH[q, o] = ER[st, q, o] * half * INV[o, 0:1, :]

        def advance(o, carry):
            inv = INV[o, 0:1, :]

            def scaled(tile):
                return U[o, :, lanes(tile)] * HALF[:, lanes(tile)] * inv

            squares = jnp.zeros((32, 128), F32)
            before = jnp.zeros((32, 128), F32)
            here = scaled(0)
            turned = pltpu.roll(here, 64, 1)
            for tile in range(32):
                if tile < 31:
                    later = scaled(tile + 1)
                    after = pltpu.roll(later, 64, 1)
                else:
                    later = here
                    after = jnp.zeros((32, 128), F32)
                next_y = pltpu.roll(jnp.where(first_y, turned, here), 127, 1)
                prior_y = pltpu.roll(jnp.where(last_y, turned, here), 1, 1)
                prior_z = jnp.where(
                    row32 == 0, SH[0, o, tile : tile + 1, :], pltpu.roll(here, 1, 0)
                )
                next_z = jnp.where(
                    row32 == 31, SH[1, o, tile : tile + 1, :], pltpu.roll(here, 31, 0)
                )
                around = turned + jnp.where(low32, before, after) + next_y + prior_y
                around = around + prior_z + next_z
                kept = 1.0 - 3.0 * TIME
                value = (kept * here + 0.5 * TIME * around) * HALF[:, lanes(tile)]
                U[o, :, lanes(tile)] = value
                EDGES[st + 1, 0, o, tile : tile + 1, :] = value[31:32]
                EDGES[st + 1, 1, o, tile : tile + 1, :] = value[0:1]
                squares = squares + value * value
                before, here, turned = turned, later, after
            NBO[o] = squares[0:8] + squares[8:16] + squares[16:24] + squares[24:32]

            @pl.when(st == STEPS - 1)
            def _():
                pltpu.make_async_copy(U.at[o], out_hbm.at[0, o], l_o.at[o]).start()

            return carry

        lax.fori_loop(0, 8, advance, 0)

        for o in range(8):
            NB[st, o : o + 1, :] = jnp.sum(NBO[o], axis=0, keepdims=True)
        norm_copy = send(NB.at[st], NR.at[st], ssN.at[st], rsN.at[st], {"sub": other})
        norm_copy.start()
        copy_a.wait_send()
        for copy in copies_b + moment_copies + side_copies + gather + forward + [copy_4, edge_copy]:
            copy.wait_send()
        norm_copy.wait()
        norms = jnp.sum(NB[st] + NR[st], axis=1, keepdims=True)
        inv = jnp.broadcast_to(1.0 / jnp.sqrt(norms / CELLS + EPS), (8, 128))
        for o in range(8):
            INV[o] = jnp.broadcast_to(inv[o : o + 1], (8, 128))
        W8[...] = OCC8[...] * inv * inv
        return carry

    lax.fori_loop(0, STEPS, step, 0)
    for o in range(8):
        inv_out[o : o + 1, :] = INV[o, 0:1, :]
    last = pltpu.make_async_copy(VB, pot_hbm.at[0], l_o.at[8])
    last.start()
    for o in range(8):
        pltpu.make_async_copy(U.at[o], out_hbm.at[0, o], l_o.at[o]).wait()
    last.wait()


def body(orbitals, occupations, ext_potential, core_range):
    consts = tables()
    hbm = pl.BlockSpec(memory_space=pl.ANY)
    smem = pl.BlockSpec(memory_space=pltpu.SMEM)
    vmem = pl.BlockSpec(memory_space=pltpu.VMEM)
    V = lambda *s: pltpu.VMEM(s, F32)
    D = lambda *s: pltpu.SemaphoreType.DMA(s)
    out, pot, inv = pl.pallas_call(
        kernel,
        out_shape=(
            jax.ShapeDtypeStruct(orbitals.shape, F32),
            jax.ShapeDtypeStruct(ext_potential.shape, F32),
            jax.ShapeDtypeStruct((8, 128), F32),
        ),
        in_specs=[hbm, smem, hbm, smem] + [hbm] * 5,
        out_specs=(hbm, hbm, vmem),
        scratch_shapes=[
            V(8, 32, 4096), V(32, 4096), V(32, 4096), V(32, 4096),
            V(128, 128), V(128, 128), V(128, 512), V(512, 512), V(11, 8, 128),
            V(8, 128), V(8, 128), V(8, 8, 128),
            V(2, 4, 16, 8, 128), V(3, 4, 16, 8, 128), V(4, 16, 8, 128), V(3, 3, 16, 8, 128),
            V(64, 8, 128), V(64, 8, 128), V(64, 8, 128),
            V(2, 8, 8, 128), V(3, 2, 8, 8, 128), V(3, 8, 8, 128), V(128, 512),
            V(2, 17, 8, 128), V(3, 17, 8, 128), V(3, 8, 17, 8, 128),
            V(4, 2, 8, 32, 128), V(3, 2, 8, 32, 128), V(2, 32, 128), V(2, 32, 128), V(2, 32, 128),
            V(2, 8, 32, 128), V(8, 8, 128), V(3, 8, 128), V(3, 8, 128),
            D(8), D(6), D(3), D(3), D(3, 3), D(3, 3), D(3, 2), D(3, 2), D(3, 7), D(3, 7),
            D(3), D(3), D(3, 3), D(3, 3), D(3, 4), D(3, 4), D(3), D(3), D(1), D(1), D(3), D(3), D(9),
        ],
        compiler_params=pltpu.CompilerParams(
            collective_id=0, has_side_effects=True, vmem_limit_bytes=60 * 1024 * 1024
        ),
        name="steps",
    )(orbitals, occupations, ext_potential, core_range, *[jnp.asarray(c) for c in consts])
    return out * inv[:, 0][None, :, None, None], pot


def solution(mesh):
    return jax.shard_map(
        body,
        mesh=mesh,
        in_specs=(
            P("dom", "band", "sub", None),
            P("dom", "band"),
            P("dom", "sub", None),
            P("dom", None),
        ),
        out_specs=(P("dom", "band", "sub", None), P("dom", "sub", None)),
        check_vma=False,
    )
```

```python
import functools

import jax
import jax.numpy as jnp
import numpy as np
from jax import lax
from jax.experimental import pallas as pl
from jax.experimental.pallas import tpu as pltpu
from jax.sharding import PartitionSpec as P

EDGE = 64
MARGIN = 8
BLOCK = 4
STEPS = 3
CORE = 48
GX = 384
N_DOM = 8
N_BAND = 8
TIME = 0.2
SCREEN = 0.02
EPS = 1e-06
CELLS = float(EDGE**3)
F32 = jnp.float32
HIGH = lax.Precision.HIGH
MESH = pl.DeviceIdType.MESH


def cas(rows, cols, n):
    angle = 2.0 * np.pi / n * ((rows[:, None] * cols[None, :]) % n)
    return np.cos(angle) + np.sin(angle)


def tables():
    ids = np.arange(EDGE)
    full = cas(ids, ids, EDGE)
    w_y = np.kron(np.eye(2), full)
    w_h = np.concatenate([np.concatenate([full, full], 1), np.zeros((64, 128))], 0)
    w_z = np.kron(np.eye(4), np.concatenate([full[:32], full[:32]], 1))
    both = np.concatenate([full, full], 0)
    halo0 = np.tile(both[:, [63, 32]], (1, 16))
    halo1 = np.tile(both[:, [31, 0]], (1, 16))
    w_i = np.concatenate(
        [np.kron(np.eye(4), b) for b in (both[:, :32], both[:, 32:], halo0, halo1)], 1
    )
    lam = 2.0 - 2.0 * np.cos(2.0 * np.pi / EDGE * ids)
    a = lam[:, None] + lam[None, :] + SCREEN
    r = 1.0 / (1.0 + a / 2 + np.sqrt(a + a * a / 4))
    scale = 1.0 / (1.0 / r - r) / (EDGE * EDGE)
    sign = np.where(ids % 2 == 1, -1.0, 1.0)[None, :]
    rows = [r, scale, scale * sign]
    for k in range(2, 10):
        rows.append(r ** (CORE * k - 63) / (1.0 - r**GX))
    modes = np.stack(rows)
    modes = np.concatenate([modes, modes], 2).reshape(11, N_BAND, 8, 128).transpose(1, 0, 2, 3)
    swap = np.kron(1.0 - np.eye(2), np.eye(64))
    ring = np.roll(np.eye(64), 1, 0) + np.roll(np.eye(64), -1, 0)
    stencil = np.concatenate([np.kron(np.eye(2), ring) + swap, swap], 1)
    stencil = np.concatenate([stencil, stencil], 0)
    out = [np.asarray(v, np.float32) for v in (w_y, w_h, w_z, w_i, modes)]
    return out + [np.asarray(stencil, jnp.bfloat16)]


def dot(a, b, dims=((1,), (0,))):
    return lax.dot_general(a, b, (dims, ((), ())), precision=HIGH, preferred_element_type=F32)


def kernel(
    orb_hbm, occ, ext_hbm, core, wy_hbm, wh_hbm, wz_hbm, wi_hbm, modes_hbm, st_hbm,
    U, VB, INV,
    HALF, EXT, WY, WH, WZ, WI, MODES, WS, OCC8, W8, SC, MX,
    SB, RA, S1, RB, S2, PP, PW, FS, FR, MV, QB, OB, R4, AG, EDGES, ER, EXTE, EXTR, HH, SH, NBO, NB, NR,
    l_u, l_c, ssA, rsA, ssB, rsB, ssF, rsF, ssM, rsM, ss4, rs4, ssG, rsG, ssH, rsH, ssE, rsE,
    ssX, rsX, ssN, rsN,
):
    d = lax.axis_index("dom")
    b = lax.axis_index("band")
    h = lax.axis_index("sub")
    zi = b // 2
    co = b % 2
    mate = zi * 2 + (1 - co)
    other = 1 - h

    def zpeer(k):
        return ((zi + k) % 4) * 2 + co

    loads = [pltpu.make_async_copy(orb_hbm.at[0, o], U.at[0, o], l_u.at[o]) for o in range(8)]
    loads += [
        pltpu.make_async_copy(src, dst, l_c.at[i])
        for i, (src, dst) in enumerate(
            (
                (wy_hbm, WY),
                (ext_hbm.at[0], EXT),
                (wh_hbm, WH),
                (wz_hbm, WZ),
                (wi_hbm, WI),
                (modes_hbm.at[b], MODES),
                (st_hbm, WS),
            )
        )
    ]
    for c in loads:
        c.start()

    barrier = pltpu.get_barrier_semaphore()

    def greet(dev):
        pl.semaphore_signal(barrier, inc=1, device_id=dev, device_id_type=MESH)

    greet({"band": mate})
    for k in range(1, 4):
        greet({"band": zpeer(k)})
    greet({"sub": other})
    for k in range(1, 8):
        greet({"dom": (d + k) % 8})

    def send(src, dst, ss, rs, dev):
        return pltpu.make_async_remote_copy(
            src_ref=src, dst_ref=dst, send_sem=ss, recv_sem=rs, device_id=dev, device_id_type=MESH
        )

    lane = lax.broadcasted_iota(jnp.int32, (8, 128), 1)
    low = lane < 64
    lane16 = lax.broadcasted_iota(jnp.int32, (16, 128), 1)
    lane32 = lax.broadcasted_iota(jnp.int32, (32, 128), 1)
    row8 = lax.broadcasted_iota(jnp.int32, (8, 128), 0)
    top = row8 == 0
    bottom = row8 == 7
    slot = (lane % 32) // 2
    zero8 = jnp.zeros((8, 128), F32)

    for o in range(8):
        OCC8[o : o + 1, :] = jnp.full((1, 128), occ[0, o], F32)
    W8[...] = OCC8[...]
    INV[...] = jnp.ones((8, 8, 128), F32)

    def lanes(tile):
        return pl.ds(tile * 128, 128)

    low_x = core[0, 0] * BLOCK
    high_x = core[0, 1] * BLOCK

    def to_mate(st, half):
        part = pl.ds(8 * half, 8)
        return send(
            SB.at[1 - co, :, part], RA.at[st, :, part], ssA.at[st, half], rsA.at[st, half],
            {"band": mate},
        )

    def edges_of(st):
        return send(EDGES.at[st], ER.at[st], ssE.at[st], rsE.at[st], {"sub": other})

    def density(st, first):
        for g in range(8):
            tiles = []
            for t in range(4):
                tile = 4 * g + t
                acc = jnp.zeros((32, 128), F32)
                for o in range(8):
                    value = U[0, o, :, lanes(tile)]
                    acc = acc + value * value * W8[o : o + 1, :]
                x = 2 * tile + lane32 // 64
                tiles.append(jnp.where((x >= low_x) & (x < high_x), acc, 0.0))
            rho = jnp.concatenate(tiles, 0)
            out = dot(WY[...], rho, ((1,), (1,)))
            for x2 in range(2):
                for c in range(2):
                    for z in range(4):
                        row = x2 * 64 + (2 * z + c) * 8
                        SB[c, z, 2 * g + x2] = out[row : row + 8]
            if g == 3 and first:
                pl.semaphore_wait(barrier, 12)
            if g % 4 == 3:
                to_mate(st, g // 4).start()

    for c in loads[:9]:
        c.wait()
    density(0, True)
    for c in loads[9:]:
        c.wait()

    for tile in range(32):
        EXTE[0, tile : tile + 1, :] = EXT[31:32, lanes(tile)]
        EXTE[1, tile : tile + 1, :] = EXT[0:1, lanes(tile)]

    def first_edges(o, carry):
        for tile in range(32):
            EDGES[0, 0, o, tile : tile + 1, :] = U[0, o, 31:32, lanes(tile)]
            EDGES[0, 1, o, tile : tile + 1, :] = U[0, o, 0:1, lanes(tile)]
        return carry

    lax.fori_loop(0, 8, first_edges, 0)
    ext_copy = send(EXTE, EXTR, ssX.at[0], rsX.at[0], {"sub": other})
    ext_copy.start()
    edges_of(0).start()

    r = MODES[0]
    power = jnp.ones((8, 128), F32)
    for i in range(64):
        PW[i] = power
        power = power * r

    def step(st, carry):
        edge_copy = edges_of(st)

        copies_a = [to_mate(st, half) for half in range(2)]
        copies_b = []
        for half in range(2):
            part = pl.ds(8 * half, 8)
            copies_a[half].wait_recv()
            for k in (2, 1, 3):
                z = (zi + k) % 4
                S1[k, part] = SB[co, z, part] + RA[st, z, part]
                copy = send(
                    S1.at[k, part], RB.at[st, k - 1, part], ssB.at[st, k - 1, half],
                    rsB.at[st, k - 1, half], {"band": zpeer(k)},
                )
                copy.start()
                copies_b.append(copy)
            S1[0, part] = SB[co, zi, part] + RA[st, zi, part]
        for copy in copies_b:
            copy.wait_recv()
        total = S1[0] + RB[st, 0] + RB[st, 1] + RB[st, 2]

        out = dot(total.reshape(128, 128), WZ[...])
        scale = MODES[1 + h]
        r = MODES[0]
        for g in range(8):
            for t in range(4):
                for x2 in range(2):
                    row = (2 * g + x2) * 8
                    S2[8 * g + 2 * t + x2] = out[row : row + 8, t * 128 : t * 128 + 128] * scale

        p = zero8
        for i in range(64):
            p = p * r + jnp.where(low, S2[i], S2[63 - i])
            PP[i] = p
        MV[st, d] = p
        moment_copies = []
        for k in range(1, 8):
            copy = send(
                MV.at[st, d], MV.at[st, d], ssM.at[st, k - 1], rsM.at[st, k - 1], {"dom": (d + k) % 8}
            )
            copy.start()
            moment_copies.append(copy)

        def response(x):
            return jnp.where(low, PP[x] - S2[x], PP[63 - x])

        side_copies = []
        for side, base, peer in ((0, 48, (d + 1) % 8), (1, 0, (d + 7) % 8)):
            for m in range(8):
                even = response(base + 2 * m)
                odd = response(base + 2 * m + 1)
                even = even + pltpu.roll(even, 64, 1)
                odd = odd + pltpu.roll(odd, 64, 1)
                FS[side, m] = jnp.where(low, even, odd)
            copy = send(
                FS.at[side], FR.at[st, side], ssF.at[st, side], rsF.at[st, side], {"dom": peer}
            )
            copy.start()
            side_copies.append(copy)

        for copy in moment_copies:
            copy.wait_recv()
        for copy in side_copies:
            copy.wait_recv()

        incoming = zero8
        for k in range(2, 10):
            moved = jnp.where(low, MV[st, (d + 16 - k) % 8], MV[st, (d + k) % 8])
            incoming = incoming + MODES[1 + k] * moved
        near = jnp.where(low, MV[st, (d + 7) % 8], MV[st, (d + 1) % 8])
        for i in range(64):
            value = PP[i] + PW[i] * incoming
            if i >= 16:
                value = value + PW[i - 15] * near
            PP[i] = value
        for x in range(64):
            value = response(x)
            if x < 16:
                part = FR[st, 0, x // 2]
                value = value + jnp.where(low if x % 2 == 0 else ~low, part, 0.0)
            if x >= 48:
                part = FR[st, 1, (x - 48) // 2]
                value = value + jnp.where(low if x % 2 == 0 else ~low, part, 0.0)
            g, t, x2 = x // 8, (x % 8) // 2, x % 2
            row = (2 * g + x2) * 8
            QB[row : row + 8, t * 128 : t * 128 + 128] = value

        out = dot(QB[...], WI[...])
        for q in range(2):
            halo = zero8
            for g in range(8):
                for x2 in range(2):
                    j = 2 * g + x2
                    OB[q, j] = out[j * 8 : j * 8 + 8, q * 128 : q * 128 + 128]
                    part = out[j * 8 : j * 8 + 8, (2 + q) * 128 : (2 + q) * 128 + 128]
                    halo = jnp.where(slot == x2 * 8 + g, part, halo)
            OB[q, 16] = halo
        parts = (pl.ds(0, 8), pl.ds(8, 9))
        copies_4 = []
        for half, part in enumerate(parts):
            copy = send(
                OB.at[other, part], R4.at[st, part], ss4.at[st, half], rs4.at[st, half], {"sub": other}
            )
            copy.start()
            copies_4.append(copy)

        gather, forward = [], []

        def pass_on(index, k, half):
            block = AG.at[st, index, parts[half]]
            copy = send(block, block, ssH.at[st, k, half], rsH.at[st, k, half], {"band": mate})
            copy.start()
            forward.append(copy)

        for half, part in enumerate(parts):
            copies_4[half].wait_recv()
            AG[st, b, part] = OB[h, part] + R4[st, part]
            block = AG.at[st, b, part]
            for k in (2, 1, 3):
                copy = send(
                    block, block, ssG.at[st, k - 1, half], rsG.at[st, k - 1, half], {"band": zpeer(k)}
                )
                copy.start()
                gather.append((k, half, copy))
            pass_on(b, 0, half)
        for half in range(2):
            for k in (1, 3, 2):
                for kk, hh, copy in gather:
                    if (kk, hh) == (k, half):
                        copy.wait_recv()
                pass_on(zpeer(4 - k), k, half)
        for copy in forward:
            copy.wait_recv()

        for g in range(8):
            parts = [AG[st, :, 2 * g + x2].reshape(64, 128) for x2 in range(2)]
            cols = jnp.concatenate(parts, 0).T
            out = dot(cols, WY[...])
            for t in range(4):
                tile = 4 * g + t
                value = out[t * 32 : t * 32 + 32]
                VB[:, lanes(tile)] = value
                HALF[:, lanes(tile)] = jnp.exp(-0.5 * TIME * (value + EXT[:, lanes(tile)]))

        @pl.when(st == 0)
        def _():
            ext_copy.wait()

        edge_copy.wait_recv()
        rims = AG[st, :, 16].reshape(64, 128)
        out = dot(jnp.concatenate([rims, rims], 0).T, WH[...])
        low16 = lane16 < 64
        for t in range(4):
            value = jnp.where(low16, out[t * 32 : t * 32 + 16], out[t * 32 + 16 : t * 32 + 32])
            for g in range(8):
                tile = 4 * g + t
                for q in range(2):
                    HH[q, tile : tile + 1, :] = value[2 * g + q : 2 * g + q + 1]
        for q in range(2):
            half = jnp.exp(-0.5 * TIME * (HH[q] + EXTR[q]))
            for o in range(8):
                SH[q, o] = ER[st, q, o] * half * INV[o, 0:1, :]

        def advance(o, carry):
            inv = INV[o, 0:1, :]
            for c in range(4):
                rows = []
                for tile in range(8 * c, 8 * c + 8):
                    here = U[0, o, :, lanes(tile)] * HALF[:, lanes(tile)] * inv
                    SC[tile] = here
                    coarse = here.astype(jnp.bfloat16)
                    fine = (here - coarse.astype(F32)).astype(jnp.bfloat16)
                    rows.append(jnp.concatenate([coarse, fine], 1))
                near = jnp.dot(jnp.concatenate(rows, 0), WS[...], preferred_element_type=F32)
                MX[8 * c : 8 * c + 8] = near.reshape(8, 32, 256)
            squares = zero8
            for tile in range(32):
                pieces = [SC[tile, 8 * i : 8 * i + 8] for i in range(4)]
                up = [SH[0, o, tile : tile + 1, :]] + [pltpu.roll(v, 1, 0) for v in pieces]
                down = [pltpu.roll(v, 7, 0) for v in pieces] + [SH[1, o, tile : tile + 1, :]]
                for i in range(4):
                    span = slice(8 * i, 8 * i + 8)
                    before = MX[tile - 1, span, 128:] if tile > 0 else zero8
                    after = MX[tile + 1, span, 128:] if tile < 31 else zero8
                    around = MX[tile, span, :128] + jnp.where(low, before, after)
                    around = around + jnp.where(top, up[i], up[i + 1])
                    around = around + jnp.where(bottom, down[i + 1], down[i])
                    kept = 1.0 - 3.0 * TIME
                    value = kept * pieces[i] + 0.5 * TIME * around
                    value = value * HALF[span, lanes(tile)]
                    U[0, o, span, lanes(tile)] = value
                    squares = squares + value * value
                    if i == 3:
                        EDGES[st + 1, 0, o, tile : tile + 1, :] = value[7:8]
                    if i == 0:
                        EDGES[st + 1, 1, o, tile : tile + 1, :] = value[0:1]
            NBO[o] = squares
            return carry

        lax.fori_loop(0, 8, advance, 0)

        for o in range(8):
            NB[st, o : o + 1, :] = jnp.sum(NBO[o], axis=0, keepdims=True)
        norm_copy = send(NB.at[st], NR.at[st], ssN.at[st], rsN.at[st], {"sub": other})
        norm_copy.start()

        @pl.when(st < STEPS - 1)
        def _():
            edges_of(st + 1).start()

        for copy in copies_a + copies_b + moment_copies + side_copies + copies_4 + forward:
            copy.wait_send()
        for _, _, copy in gather:
            copy.wait_send()
        edge_copy.wait_send()
        norm_copy.wait()
        norms = jnp.sum(NB[st] + NR[st], axis=1, keepdims=True)
        inv = jnp.broadcast_to(1.0 / jnp.sqrt(norms / CELLS + EPS), (8, 128))
        for o in range(8):
            INV[o] = jnp.broadcast_to(inv[o : o + 1], (8, 128))
        W8[...] = OCC8[...] * inv * inv

        @pl.when(st < STEPS - 1)
        def _():
            density(st + 1, False)

        return carry

    lax.fori_loop(0, STEPS, step, 0)


def scale_out(U, VB, INV, out_hbm, pot_hbm, buffer, sems):
    copies = [pltpu.make_async_copy(VB, pot_hbm.at[0], sems.at[8])]
    copies[0].start()
    for o in range(8):
        for tile in range(32):
            lanes = pl.ds(tile * 128, 128)
            buffer[o, :, lanes] = U[0, o, :, lanes] * INV[o, 0:1, :]
        copy = pltpu.make_async_copy(buffer.at[o], out_hbm.at[0, o], sems.at[o])
        copy.start()
        copies.append(copy)
    for copy in copies:
        copy.wait()


def body(orbitals, occupations, ext_potential, core_range):
    operands = [orbitals, occupations, ext_potential, core_range]
    operands += [jnp.asarray(c) for c in tables()]
    hbm = pl.BlockSpec(memory_space=pltpu.HBM)
    smem = pl.BlockSpec(memory_space=pltpu.SMEM)
    vmem = pl.BlockSpec(memory_space=pltpu.VMEM)
    V = lambda *s: pltpu.VMEM(s, F32)
    D = lambda *s: pltpu.SemaphoreType.DMA(s)
    state, pot, inv = pl.pallas_call(
        kernel,
        out_shape=(
            pltpu.VMEM(orbitals.shape, F32),
            pltpu.VMEM(ext_potential.shape[1:], F32),
            pltpu.VMEM((8, 8, 128), F32),
        ),
        in_specs=[hbm, smem, hbm, smem] + [hbm] * 6,
        out_specs=(vmem, vmem, vmem),
        scratch_shapes=[
            V(32, 4096), V(32, 4096),
            V(128, 128), V(128, 128), V(128, 512), V(512, 512), V(11, 8, 128),
            pltpu.VMEM((256, 256), jnp.bfloat16),
            V(8, 128), V(8, 128), V(32, 32, 128), V(32, 32, 256),
            V(2, 4, 16, 8, 128), V(3, 4, 16, 8, 128), V(4, 16, 8, 128), V(3, 3, 16, 8, 128),
            V(64, 8, 128), V(64, 8, 128), V(64, 8, 128),
            V(2, 8, 8, 128), V(3, 2, 8, 8, 128), V(3, 8, 8, 128), V(128, 512),
            V(2, 17, 8, 128), V(3, 17, 8, 128), V(3, 8, 17, 8, 128),
            V(4, 2, 8, 32, 128), V(3, 2, 8, 32, 128), V(2, 32, 128), V(2, 32, 128), V(2, 32, 128),
            V(2, 8, 32, 128), V(8, 8, 128), V(3, 8, 128), V(3, 8, 128),
            D(8), D(7), D(3, 2), D(3, 2), D(3, 3, 2), D(3, 3, 2), D(3, 2), D(3, 2), D(3, 7), D(3, 7),
            D(3, 2), D(3, 2), D(3, 3, 2), D(3, 3, 2), D(3, 4, 2), D(3, 4, 2),
            D(3), D(3), D(1), D(1), D(3), D(3),
        ],
        compiler_params=pltpu.CompilerParams(
            collective_id=0, has_side_effects=True, vmem_limit_bytes=59 * 1024 * 1024
        ),
        name="steps",
    )(
        *[
            v if i in (1, 3) else pltpu.with_memory_space_constraint(v, pltpu.HBM)
            for i, v in enumerate(operands)
        ]
    )
    return pl.pallas_call(
        scale_out,
        out_shape=(
            jax.ShapeDtypeStruct(orbitals.shape, F32),
            jax.ShapeDtypeStruct(ext_potential.shape, F32),
        ),
        in_specs=[vmem] * 3,
        out_specs=(hbm, hbm),
        scratch_shapes=[V(8, 32, 4096), D(9)],
        compiler_params=pltpu.CompilerParams(vmem_limit_bytes=8 * 1024 * 1024),
        name="scale_out",
    )(state, pot, inv)


def solution(mesh):
    return jax.shard_map(
        body,
        mesh=mesh,
        in_specs=(
            P("dom", "band", "sub", None),
            P("dom", "band"),
            P("dom", "sub", None),
            P("dom", None),
        ),
        out_specs=(P("dom", "band", "sub", None), P("dom", "sub", None)),
        check_vma=False,
    )
```

```python
import functools

import jax
import jax.numpy as jnp
import numpy as np
from jax import lax
from jax.experimental import pallas as pl
from jax.experimental.pallas import tpu as pltpu
from jax.sharding import PartitionSpec as P

EDGE = 64
MARGIN = 8
BLOCK = 4
STEPS = 3
CORE = 48
GX = 384
N_DOM = 8
N_BAND = 8
TIME = 0.2
SCREEN = 0.02
EPS = 1e-06
CELLS = float(EDGE**3)
F32 = jnp.float32
HIGH = lax.Precision.HIGH
MESH = pl.DeviceIdType.MESH


def cas(rows, cols, n):
    angle = 2.0 * np.pi / n * ((rows[:, None] * cols[None, :]) % n)
    return np.cos(angle) + np.sin(angle)


def tables():
    ids = np.arange(EDGE)
    full = cas(ids, ids, EDGE)
    w_y = np.kron(np.eye(2), full)
    w_h = np.concatenate([np.concatenate([full, full], 1), np.zeros((64, 128))], 0)
    w_z = np.kron(np.eye(4), np.concatenate([full[:32], full[:32]], 1))
    both = np.concatenate([full, full], 0)
    halo0 = np.tile(both[:, [63, 32]], (1, 16))
    halo1 = np.tile(both[:, [31, 0]], (1, 16))
    w_i = [np.kron(np.eye(4), v) for v in (both[:, :32], halo0, both[:, 32:], halo1)]
    w_i = np.stack([np.concatenate(w_i[:2], 1), np.concatenate(w_i[2:], 1)])
    lam = 2.0 - 2.0 * np.cos(2.0 * np.pi / EDGE * ids)
    a = lam[:, None] + lam[None, :] + SCREEN
    r = 1.0 / (1.0 + a / 2 + np.sqrt(a + a * a / 4))
    scale = 1.0 / (1.0 / r - r) / (EDGE * EDGE)
    sign = np.where(ids % 2 == 1, -1.0, 1.0)[None, :]
    rows = [r, scale, scale * sign]
    for k in range(2, 10):
        rows.append(r ** (CORE * k - 63) / (1.0 - r**GX))
    modes = np.stack(rows)
    modes = np.concatenate([modes, modes], 2).reshape(11, N_BAND, 8, 128).transpose(1, 0, 2, 3)
    swap = np.kron(1.0 - np.eye(2), np.eye(64))
    ring = np.roll(np.eye(64), 1, 0) + np.roll(np.eye(64), -1, 0)
    stencil = np.concatenate([np.kron(np.eye(2), ring) + swap, swap], 1)
    stencil = np.concatenate([stencil, stencil], 0)
    out = [np.asarray(v, np.float32) for v in (w_y, w_h, w_z, w_i, modes)]
    return out + [np.asarray(stencil, jnp.bfloat16)]


def dot(a, b, dims=((1,), (0,))):
    return lax.dot_general(a, b, (dims, ((), ())), precision=HIGH, preferred_element_type=F32)


def kernel(
    orb_hbm, occ, ext_hbm, core, wy_hbm, wh_hbm, wz_hbm, wi_hbm, modes_hbm, st_hbm,
    U, VB, INV,
    HALF, EXT, WY, WH, WZ, WI, MODES, WS, OCC8, W8, SC, MX,
    SB, RA, S1, RB, S2, S3, ST, PP, P2, PW, FR, MV, QB, OB, R4, AG, EDGES, ER, EXTE, EXTR, HH, SH, NBO, NB, NR,
    l_u, l_c, ssA, rsA, ssB, rsB, ssF, rsF, ssM, rsM, ss4, rs4, ssG, rsG, ssH, rsH, ssE, rsE,
    ssX, rsX, ssN, rsN,
):
    d = lax.axis_index("dom")
    b = lax.axis_index("band")
    h = lax.axis_index("sub")
    zi = b // 2
    co = b % 2
    mate = zi * 2 + (1 - co)
    other = 1 - h

    def zpeer(k):
        return ((zi + k) % 4) * 2 + co

    loads = [pltpu.make_async_copy(orb_hbm.at[0, o], U.at[0, o], l_u.at[o]) for o in range(8)]
    loads += [
        pltpu.make_async_copy(src, dst, l_c.at[i])
        for i, (src, dst) in enumerate(
            (
                (wy_hbm, WY),
                (ext_hbm.at[0], EXT),
                (wh_hbm, WH),
                (wz_hbm, WZ),
                (wi_hbm, WI),
                (modes_hbm.at[b], MODES),
                (st_hbm, WS),
            )
        )
    ]
    for c in loads:
        c.start()

    barrier = pltpu.get_barrier_semaphore()

    def greet(dev):
        pl.semaphore_signal(barrier, inc=1, device_id=dev, device_id_type=MESH)

    greet({"band": mate})
    for k in range(1, 4):
        greet({"band": zpeer(k)})
    greet({"sub": other})
    for k in range(1, 8):
        for sub in (h, other):
            greet({"dom": (d + k) % 8, "sub": sub})

    def send(src, dst, ss, rs, dev):
        return pltpu.make_async_remote_copy(
            src_ref=src, dst_ref=dst, send_sem=ss, recv_sem=rs, device_id=dev, device_id_type=MESH
        )

    lane = lax.broadcasted_iota(jnp.int32, (8, 128), 1)
    low = lane < 64
    lane16 = lax.broadcasted_iota(jnp.int32, (16, 128), 1)
    lane32 = lax.broadcasted_iota(jnp.int32, (32, 128), 1)
    row8 = lax.broadcasted_iota(jnp.int32, (8, 128), 0)
    top = row8 == 0
    bottom = row8 == 7
    slot = (lane % 32) // 2
    zero8 = jnp.zeros((8, 128), F32)

    for o in range(8):
        OCC8[o : o + 1, :] = jnp.full((1, 128), occ[0, o], F32)
    W8[...] = OCC8[...]
    INV[...] = jnp.ones((8, 8, 128), F32)

    def lanes(tile):
        return pl.ds(tile * 128, 128)

    low_x = core[0, 0] * BLOCK
    high_x = core[0, 1] * BLOCK

    def to_mate(st, half):
        part = pl.ds(8 * half, 8)
        return send(
            SB.at[1 - co, :, part], RA.at[st, :, part], ssA.at[st, half], rsA.at[st, half],
            {"band": mate},
        )

    def edges_of(st):
        return send(EDGES.at[st], ER.at[st], ssE.at[st], rsE.at[st], {"sub": other})

    def density(st, first):
        for g in range(8):
            tiles = []
            for t in range(4):
                tile = 4 * g + t
                acc = jnp.zeros((32, 128), F32)
                for o in range(8):
                    value = U[0, o, :, lanes(tile)]
                    acc = acc + value * value * W8[o : o + 1, :]
                x = 2 * tile + lane32 // 64
                tiles.append(jnp.where((x >= low_x) & (x < high_x), acc, 0.0))
            rho = jnp.concatenate(tiles, 0)
            out = dot(WY[...], rho, ((1,), (1,)))
            for x2 in range(2):
                for c in range(2):
                    for z in range(4):
                        row = x2 * 64 + (2 * z + c) * 8
                        SB[c, z, 2 * g + x2] = out[row : row + 8]
            if g == 3 and first:
                pl.semaphore_wait(barrier, 19)
            if g % 4 == 3:
                to_mate(st, g // 4).start()

    for c in loads[:9]:
        c.wait()
    density(0, True)
    for c in loads[9:]:
        c.wait()

    for tile in range(32):
        EXTE[0, tile : tile + 1, :] = EXT[31:32, lanes(tile)]
        EXTE[1, tile : tile + 1, :] = EXT[0:1, lanes(tile)]

    def first_edges(o, carry):
        for tile in range(32):
            EDGES[0, 0, o, tile : tile + 1, :] = U[0, o, 31:32, lanes(tile)]
            EDGES[0, 1, o, tile : tile + 1, :] = U[0, o, 0:1, lanes(tile)]
        return carry

    lax.fori_loop(0, 8, first_edges, 0)
    ext_copy = send(EXTE, EXTR, ssX.at[0], rsX.at[0], {"sub": other})
    ext_copy.start()
    edges_of(0).start()

    r = MODES[0]
    power = jnp.ones((8, 128), F32)
    for i in range(64):
        PW[i] = power
        power = power * r

    def step(st, carry):
        edge_copy = edges_of(st)

        copies_a = [to_mate(st, half) for half in range(2)]
        copies_b = []
        for half in range(2):
            part = pl.ds(8 * half, 8)
            copies_a[half].wait_recv()
            for k in (2, 1, 3):
                z = (zi + k) % 4
                S1[k, part] = SB[co, z, part] + RA[st, z, part]
                copy = send(
                    S1.at[k, part], RB.at[st, k - 1, part], ssB.at[st, k - 1, half],
                    rsB.at[st, k - 1, half], {"band": zpeer(k)},
                )
                copy.start()
                copies_b.append(copy)
            S1[0, part] = SB[co, zi, part] + RA[st, zi, part]
        for copy in copies_b:
            copy.wait_recv()
        ST[...] = S1[0] + RB[st, 0] + RB[st, 1] + RB[st, 2]

        dom_copies = []
        for side, part, peer in ((0, pl.ds(12, 4), (d + 1) % 8), (1, pl.ds(0, 4), (d + 7) % 8)):
            for i, sub in enumerate((h, other)):
                copy = send(
                    ST.at[part], FR.at[st, h, side], ssF.at[st, i, side], rsF.at[st, h, side],
                    {"dom": peer, "sub": sub},
                )
                copy.start()
                dom_copies.append(copy)

        out = dot(ST[...].reshape(128, 128), WZ[...])
        scale = MODES[1 + h]
        r = MODES[0]
        for g in range(8):
            for t in range(4):
                for x2 in range(2):
                    row = (2 * g + x2) * 8
                    S2[8 * g + 2 * t + x2] = out[row : row + 8, t * 128 : t * 128 + 128] * scale

        p = zero8
        for i in range(64):
            p = p * r + jnp.where(low, S2[i], S2[63 - i])
            PP[i] = p
            if i == 47:
                MV[st, h, d, 0] = p
        MV[st, h, d, 1] = p
        mine = MV.at[st, h, d]
        for k in range(8):
            for i, sub in enumerate((h, other)):
                if k + i > 0:
                    copy = send(
                        mine, mine, ssM.at[st, i, k], rsM.at[st, h, k],
                        {"dom": (d + k) % 8, "sub": sub},
                    )
                    copy.start()
                    dom_copies.append(copy)

        def place(x, value):
            row = (2 * (x // 8) + x % 2) * 8
            t = (x % 8) // 2
            QB[row : row + 8, t * 128 : t * 128 + 128] = value

        def planes(q, put):
            out = dot(QB[...], WI[q])
            halo = zero8
            for g in range(8):
                for x2 in range(2):
                    j = 2 * g + x2
                    put(j, out[j * 8 : j * 8 + 8, :128])
                    part = out[j * 8 : j * 8 + 8, 128:]
                    halo = jnp.where(slot == x2 * 8 + g, part, halo)
            put(16, halo)

        for x in range(64):
            place(x, jnp.where(low, PP[x] - S2[x], PP[63 - x]))

        def to_other(j, value):
            OB[j] = value

        planes(other, to_other)
        copy_4 = send(OB, R4.at[st], ss4.at[st], rs4.at[st], {"sub": other})
        copy_4.start()

        def arrived(sub, index, sems, where):
            return send(where, where, sems.at[st, sub, index], sems.at[st, sub, index], {"sub": other})

        for side in range(2):
            for sub in range(2):
                arrived(sub, side, rsF, FR.at[st, sub, side]).wait_recv()
        out = dot(FR[st].reshape(128, 128), WZ[...])
        for side in range(2):
            for j in range(4):
                for t in range(4):
                    row = (side * 4 + j) * 8
                    span = slice(t * 128, t * 128 + 128)
                    value = out[row : row + 8, span] * MODES[1]
                    value = value + out[row + 64 : row + 72, span] * MODES[2]
                    S3[side * 16 + 8 * (j // 2) + 2 * t + j % 2] = value
        p = zero8
        for i in range(64):
            p = p * r
            if i < 16:
                p = p + jnp.where(low, S3[i], S3[31 - i])
            if i >= 48:
                p = p + jnp.where(low, S3[i - 32], S3[63 - i])
            P2[i] = PP[i] + p

        for k in range(8):
            for i, sub in enumerate((h, other)):
                if k + i > 0:
                    arrived(sub, k, rsM, MV.at[st, sub, (d + 8 - k) % 8]).wait_recv()

        def moment(k, which):
            left, right = (d + 16 - k) % 8, (d + k) % 8
            return jnp.where(
                low,
                MV[st, 0, left, which] + MV[st, 1, left, which],
                MV[st, 0, right, which] + MV[st, 1, right, which],
            )

        incoming = r * moment(1, 0)
        for k in range(2, 10):
            incoming = incoming + MODES[1 + k] * moment(k, 1)
        for x in range(64):
            source = S2[x]
            if x < 16:
                source = source + S3[x]
            if x >= 48:
                source = source + S3[x - 32]
            forth = P2[x] + PW[x] * incoming
            back = P2[63 - x] + PW[63 - x] * incoming
            place(x, jnp.where(low, forth - source, back))
        copy_4.wait_recv()

        def to_band(j, value):
            AG[st, b, j] = value + R4[st, j]

        planes(h, to_band)
        parts = (pl.ds(0, 8), pl.ds(8, 9))

        gather, forward = [], []

        def pass_on(index, k, half):
            block = AG.at[st, index, parts[half]]
            copy = send(block, block, ssH.at[st, k, half], rsH.at[st, k, half], {"band": mate})
            copy.start()
            forward.append(copy)

        for half, part in enumerate(parts):
            block = AG.at[st, b, part]
            for k in (2, 1, 3):
                copy = send(
                    block, block, ssG.at[st, k - 1, half], rsG.at[st, k - 1, half], {"band": zpeer(k)}
                )
                copy.start()
                gather.append((k, half, copy))
            pass_on(b, 0, half)
        for half in range(2):
            for k in (1, 3, 2):
                for kk, hh, copy in gather:
                    if (kk, hh) == (k, half):
                        copy.wait_recv()
                pass_on(zpeer(4 - k), k, half)
        for copy in forward:
            copy.wait_recv()

        for g in range(8):
            parts = [AG[st, :, 2 * g + x2].reshape(64, 128) for x2 in range(2)]
            cols = jnp.concatenate(parts, 0).T
            out = dot(cols, WY[...])
            for t in range(4):
                tile = 4 * g + t
                value = out[t * 32 : t * 32 + 32]
                VB[:, lanes(tile)] = value
                HALF[:, lanes(tile)] = jnp.exp(-0.5 * TIME * (value + EXT[:, lanes(tile)]))

        @pl.when(st == 0)
        def _():
            ext_copy.wait()

        edge_copy.wait_recv()
        rims = AG[st, :, 16].reshape(64, 128)
        out = dot(jnp.concatenate([rims, rims], 0).T, WH[...])
        low16 = lane16 < 64
        for t in range(4):
            value = jnp.where(low16, out[t * 32 : t * 32 + 16], out[t * 32 + 16 : t * 32 + 32])
            for g in range(8):
                tile = 4 * g + t
                for q in range(2):
                    HH[q, tile : tile + 1, :] = value[2 * g + q : 2 * g + q + 1]
        for q in range(2):
            half = jnp.exp(-0.5 * TIME * (HH[q] + EXTR[q]))
            for o in range(8):
                SH[q, o] = ER[st, q, o] * half * INV[o, 0:1, :]

        def advance(o, carry):
            inv = INV[o, 0:1, :]
            for c in range(4):
                rows = []
                for tile in range(8 * c, 8 * c + 8):
                    here = U[0, o, :, lanes(tile)] * HALF[:, lanes(tile)] * inv
                    SC[tile] = here
                    coarse = here.astype(jnp.bfloat16)
                    fine = (here - coarse.astype(F32)).astype(jnp.bfloat16)
                    rows.append(jnp.concatenate([coarse, fine], 1))
                near = jnp.dot(jnp.concatenate(rows, 0), WS[...], preferred_element_type=F32)
                MX[8 * c : 8 * c + 8] = near.reshape(8, 32, 256)
            squares = zero8
            for tile in range(32):
                pieces = [SC[tile, 8 * i : 8 * i + 8] for i in range(4)]
                up = [SH[0, o, tile : tile + 1, :]] + [pltpu.roll(v, 1, 0) for v in pieces]
                down = [pltpu.roll(v, 7, 0) for v in pieces] + [SH[1, o, tile : tile + 1, :]]
                for i in range(4):
                    span = slice(8 * i, 8 * i + 8)
                    before = MX[tile - 1, span, 128:] if tile > 0 else zero8
                    after = MX[tile + 1, span, 128:] if tile < 31 else zero8
                    around = MX[tile, span, :128] + jnp.where(low, before, after)
                    around = around + jnp.where(top, up[i], up[i + 1])
                    around = around + jnp.where(bottom, down[i + 1], down[i])
                    kept = 1.0 - 3.0 * TIME
                    value = kept * pieces[i] + 0.5 * TIME * around
                    value = value * HALF[span, lanes(tile)]
                    U[0, o, span, lanes(tile)] = value
                    squares = squares + value * value
                    if i == 3:
                        EDGES[st + 1, 0, o, tile : tile + 1, :] = value[7:8]
                    if i == 0:
                        EDGES[st + 1, 1, o, tile : tile + 1, :] = value[0:1]
            NBO[o] = squares
            return carry

        lax.fori_loop(0, 8, advance, 0)

        for o in range(8):
            NB[st, o : o + 1, :] = jnp.sum(NBO[o], axis=0, keepdims=True)
        norm_copy = send(NB.at[st], NR.at[st], ssN.at[st], rsN.at[st], {"sub": other})
        norm_copy.start()

        @pl.when(st < STEPS - 1)
        def _():
            edges_of(st + 1).start()

        for copy in copies_a + copies_b + dom_copies + [copy_4] + forward:
            copy.wait_send()
        for _, _, copy in gather:
            copy.wait_send()
        edge_copy.wait_send()
        norm_copy.wait()
        norms = jnp.sum(NB[st] + NR[st], axis=1, keepdims=True)
        inv = jnp.broadcast_to(1.0 / jnp.sqrt(norms / CELLS + EPS), (8, 128))
        for o in range(8):
            INV[o] = jnp.broadcast_to(inv[o : o + 1], (8, 128))
        W8[...] = OCC8[...] * inv * inv

        @pl.when(st < STEPS - 1)
        def _():
            density(st + 1, False)

        return carry

    lax.fori_loop(0, STEPS, step, 0)


def scale_out(U, VB, INV, out_hbm, pot_hbm, buffer, sems):
    copies = [pltpu.make_async_copy(VB, pot_hbm.at[0], sems.at[8])]
    copies[0].start()
    for o in range(8):
        for tile in range(32):
            lanes = pl.ds(tile * 128, 128)
            buffer[o, :, lanes] = U[0, o, :, lanes] * INV[o, 0:1, :]
        copy = pltpu.make_async_copy(buffer.at[o], out_hbm.at[0, o], sems.at[o])
        copy.start()
        copies.append(copy)
    for copy in copies:
        copy.wait()


def body(orbitals, occupations, ext_potential, core_range):
    operands = [orbitals, occupations, ext_potential, core_range]
    operands += [jnp.asarray(c) for c in tables()]
    hbm = pl.BlockSpec(memory_space=pltpu.HBM)
    smem = pl.BlockSpec(memory_space=pltpu.SMEM)
    vmem = pl.BlockSpec(memory_space=pltpu.VMEM)
    V = lambda *s: pltpu.VMEM(s, F32)
    D = lambda *s: pltpu.SemaphoreType.DMA(s)
    state, pot, inv = pl.pallas_call(
        kernel,
        out_shape=(
            pltpu.VMEM(orbitals.shape, F32),
            pltpu.VMEM(ext_potential.shape[1:], F32),
            pltpu.VMEM((8, 8, 128), F32),
        ),
        in_specs=[hbm, smem, hbm, smem] + [hbm] * 6,
        out_specs=(vmem, vmem, vmem),
        scratch_shapes=[
            V(32, 4096), V(32, 4096),
            V(128, 128), V(128, 128), V(128, 512), V(2, 512, 256), V(11, 8, 128),
            pltpu.VMEM((256, 256), jnp.bfloat16),
            V(8, 128), V(8, 128), V(32, 32, 128), V(32, 32, 256),
            V(2, 4, 16, 8, 128), V(3, 4, 16, 8, 128), V(4, 16, 8, 128), V(3, 3, 16, 8, 128),
            V(64, 8, 128), V(32, 8, 128), V(16, 8, 128), V(64, 8, 128), V(64, 8, 128), V(64, 8, 128),
            V(3, 2, 2, 4, 8, 128), V(3, 2, 8, 2, 8, 128), V(128, 512),
            V(17, 8, 128), V(3, 17, 8, 128), V(3, 8, 17, 8, 128),
            V(4, 2, 8, 32, 128), V(3, 2, 8, 32, 128), V(2, 32, 128), V(2, 32, 128), V(2, 32, 128),
            V(2, 8, 32, 128), V(8, 8, 128), V(3, 8, 128), V(3, 8, 128),
            D(8), D(7), D(3, 2), D(3, 2), D(3, 3, 2), D(3, 3, 2), D(3, 2, 2), D(3, 2, 2), D(3, 2, 8), D(3, 2, 8),
            D(3), D(3), D(3, 3, 2), D(3, 3, 2), D(3, 4, 2), D(3, 4, 2),
            D(3), D(3), D(1), D(1), D(3), D(3),
        ],
        compiler_params=pltpu.CompilerParams(
            collective_id=0, has_side_effects=True, vmem_limit_bytes=59 * 1024 * 1024
        ),
        name="steps",
    )(
        *[
            v if i in (1, 3) else pltpu.with_memory_space_constraint(v, pltpu.HBM)
            for i, v in enumerate(operands)
        ]
    )
    return pl.pallas_call(
        scale_out,
        out_shape=(
            jax.ShapeDtypeStruct(orbitals.shape, F32),
            jax.ShapeDtypeStruct(ext_potential.shape, F32),
        ),
        in_specs=[vmem] * 3,
        out_specs=(hbm, hbm),
        scratch_shapes=[V(8, 32, 4096), D(9)],
        compiler_params=pltpu.CompilerParams(vmem_limit_bytes=8 * 1024 * 1024),
        name="scale_out",
    )(state, pot, inv)


def solution(mesh):
    return jax.shard_map(
        body,
        mesh=mesh,
        in_specs=(
            P("dom", "band", "sub", None),
            P("dom", "band"),
            P("dom", "sub", None),
            P("dom", None),
        ),
        out_specs=(P("dom", "band", "sub", None), P("dom", "sub", None)),
        check_vma=False,
    )
```

```python
import functools

import jax
import jax.numpy as jnp
import numpy as np
from jax import lax
from jax.experimental import pallas as pl
from jax.experimental.pallas import tpu as pltpu
from jax.sharding import PartitionSpec as P

EDGE = 64
MARGIN = 8
BLOCK = 4
STEPS = 3
CORE = 48
GX = 384
N_DOM = 8
N_BAND = 8
TIME = 0.2
SCREEN = 0.02
EPS = 1e-06
CELLS = float(EDGE**3)
F32 = jnp.float32
HIGH = lax.Precision.HIGH
MESH = pl.DeviceIdType.MESH


def cas(rows, cols, n):
    angle = 2.0 * np.pi / n * ((rows[:, None] * cols[None, :]) % n)
    return np.cos(angle) + np.sin(angle)


def tables():
    ids = np.arange(EDGE)
    full = cas(ids, ids, EDGE)
    w_y = np.kron(np.eye(2), full)
    w_h = np.concatenate([np.concatenate([full, full], 1), np.zeros((64, 128))], 0)
    w_z = np.kron(np.eye(4), np.concatenate([full[:32], full[:32]], 1))
    both = np.concatenate([full, full], 0)
    halo0 = np.tile(both[:, [63, 32]], (1, 16))
    halo1 = np.tile(both[:, [31, 0]], (1, 16))
    w_i = [np.kron(np.eye(4), v) for v in (both[:, :32], halo0, both[:, 32:], halo1)]
    w_i = np.stack([np.concatenate(w_i[:2], 1), np.concatenate(w_i[2:], 1)])
    lam = 2.0 - 2.0 * np.cos(2.0 * np.pi / EDGE * ids)
    a = lam[:, None] + lam[None, :] + SCREEN
    r = 1.0 / (1.0 + a / 2 + np.sqrt(a + a * a / 4))
    scale = 1.0 / (1.0 / r - r) / (EDGE * EDGE)
    sign = np.where(ids % 2 == 1, -1.0, 1.0)[None, :]
    rows = [r, scale, scale * sign]
    for k in range(2, 10):
        rows.append(r ** (CORE * k - 63) / (1.0 - r**GX))
    modes = np.stack(rows)
    modes = np.concatenate([modes, modes], 2).reshape(11, N_BAND, 8, 128).transpose(1, 0, 2, 3)
    swap = np.kron(1.0 - np.eye(2), np.eye(64))
    ring = np.roll(np.eye(64), 1, 0) + np.roll(np.eye(64), -1, 0)
    ring = ring + (1.0 / (0.5 * TIME) - 6.0) * np.eye(64)
    stencil = np.concatenate([np.kron(np.eye(2), ring) + swap, swap], 1)
    stencil = np.concatenate([stencil, stencil], 0)
    out = [np.asarray(v, np.float32) for v in (w_y, w_h, w_z, w_i, modes)]
    return out + [np.asarray(stencil, jnp.bfloat16)]


def dot(a, b, dims=((1,), (0,))):
    return lax.dot_general(a, b, (dims, ((), ())), precision=HIGH, preferred_element_type=F32)


def kernel(
    orb_hbm, occ, ext_hbm, core, wy_hbm, wh_hbm, wz_hbm, wi_hbm, modes_hbm, st_hbm,
    U, VB, INV,
    HALF, HT, EXT, WY, WH, WZ, WI, MODES, WS, OCC8, W8, SC, MX,
    SB, RA, S1, RB, S2, S3, ST, PP, P2, PW, FR, MV, QB, OB, R4, AG, EDGES, ER, EXTE, EXTR, HH, SH, NBO, NB, NR,
    l_u, l_c, ssA, rsA, ssB, rsB, ssF, rsF, ssM, rsM, ss4, rs4, ssG, rsG, ssH, rsH, ssE, rsE,
    ssX, rsX, ssN, rsN,
):
    d = lax.axis_index("dom")
    b = lax.axis_index("band")
    h = lax.axis_index("sub")
    zi = b // 2
    co = b % 2
    mate = zi * 2 + (1 - co)
    other = 1 - h

    def zpeer(k):
        return ((zi + k) % 4) * 2 + co

    loads = [
        pltpu.make_async_copy(
            orb_hbm.at[0, o, :, pl.ds(2048 * half, 2048)],
            U.at[0, o, :, pl.ds(2048 * half, 2048)],
            l_u.at[half, o],
        )
        for half in range(2)
        for o in range(8)
    ]
    consts = [
        pltpu.make_async_copy(src, dst, l_c.at[i])
        for i, (src, dst) in enumerate(
            (
                (wy_hbm, WY),
                (ext_hbm.at[0], EXT),
                (wh_hbm, WH),
                (wz_hbm, WZ),
                (wi_hbm, WI),
                (modes_hbm.at[b], MODES),
                (st_hbm, WS),
            )
        )
    ]
    for c in consts[:1] + loads:
        c.start()

    barrier = pltpu.get_barrier_semaphore()

    def greet(dev):
        pl.semaphore_signal(barrier, inc=1, device_id=dev, device_id_type=MESH)

    greet({"band": mate})
    for k in range(1, 4):
        greet({"band": zpeer(k)})
    greet({"sub": other})
    for k in range(1, 8):
        for sub in (h, other):
            greet({"dom": (d + k) % 8, "sub": sub})

    def send(src, dst, ss, rs, dev):
        return pltpu.make_async_remote_copy(
            src_ref=src, dst_ref=dst, send_sem=ss, recv_sem=rs, device_id=dev, device_id_type=MESH
        )

    lane = lax.broadcasted_iota(jnp.int32, (8, 128), 1)
    low = lane < 64
    lane16 = lax.broadcasted_iota(jnp.int32, (16, 128), 1)
    lane32 = lax.broadcasted_iota(jnp.int32, (32, 128), 1)
    slot = (lane % 32) // 2
    zero8 = jnp.zeros((8, 128), F32)

    for o in range(8):
        OCC8[o : o + 1, :] = jnp.full((1, 128), occ[0, o], F32)
    W8[...] = OCC8[...]
    INV[...] = jnp.ones((8, 8, 128), F32)

    def lanes(tile):
        return pl.ds(tile * 128, 128)

    low_x = core[0, 0] * BLOCK
    high_x = core[0, 1] * BLOCK

    def to_mate(st, half):
        part = pl.ds(8 * half, 8)
        return send(
            SB.at[1 - co, :, part], RA.at[st, :, part], ssA.at[st, half], rsA.at[st, half],
            {"band": mate},
        )

    def edges_of(st):
        return send(EDGES.at[st], ER.at[st], ssE.at[st], rsE.at[st], {"sub": other})

    def density(st, first):
        for g in range(8):
            if first and g % 4 == 0:
                for c in loads[2 * g : 2 * g + 8]:
                    c.wait()
            tiles = []
            for t in range(4):
                tile = 4 * g + t
                acc = jnp.zeros((32, 128), F32)
                for o in range(8):
                    value = U[0, o, :, lanes(tile)]
                    acc = acc + value * value * W8[o : o + 1, :]
                x = 2 * tile + lane32 // 64
                tiles.append(jnp.where((x >= low_x) & (x < high_x), acc, 0.0))
            rho = jnp.concatenate(tiles, 0)
            out = dot(WY[...], rho, ((1,), (1,)))
            for x2 in range(2):
                for c in range(2):
                    for z in range(4):
                        row = x2 * 64 + (2 * z + c) * 8
                        SB[c, z, 2 * g + x2] = out[row : row + 8]
            if g == 3 and first:
                pl.semaphore_wait(barrier, 19)
            if g % 4 == 3:
                to_mate(st, g // 4).start()

    consts[0].wait()
    for c in consts[1:]:
        c.start()
    density(0, True)
    for c in consts[1:]:
        c.wait()

    for tile in range(32):
        EXTE[0, tile : tile + 1, :] = EXT[31:32, lanes(tile)]
        EXTE[1, tile : tile + 1, :] = EXT[0:1, lanes(tile)]

    def first_edges(o, carry):
        for tile in range(32):
            EDGES[0, 0, o, tile : tile + 1, :] = U[0, o, 31:32, lanes(tile)]
            EDGES[0, 1, o, tile : tile + 1, :] = U[0, o, 0:1, lanes(tile)]
        return carry

    lax.fori_loop(0, 8, first_edges, 0)
    ext_copy = send(EXTE, EXTR, ssX.at[0], rsX.at[0], {"sub": other})
    ext_copy.start()
    edges_of(0).start()

    r = MODES[0]
    power = jnp.ones((8, 128), F32)
    for i in range(64):
        PW[i] = power
        power = power * r

    def step(st, carry):
        edge_copy = edges_of(st)

        copies_a = [to_mate(st, half) for half in range(2)]
        copies_b = []
        for half in range(2):
            part = pl.ds(8 * half, 8)
            copies_a[half].wait_recv()
            for k in (2, 1, 3):
                z = (zi + k) % 4
                S1[k, part] = SB[co, z, part] + RA[st, z, part]
                copy = send(
                    S1.at[k, part], RB.at[st, k - 1, part], ssB.at[st, k - 1, half],
                    rsB.at[st, k - 1, half], {"band": zpeer(k)},
                )
                copy.start()
                copies_b.append(copy)
            S1[0, part] = SB[co, zi, part] + RA[st, zi, part]
        for copy in copies_b:
            copy.wait_recv()
        ST[...] = S1[0] + RB[st, 0] + RB[st, 1] + RB[st, 2]

        dom_copies = []
        for side, part, peer in ((0, pl.ds(12, 4), (d + 1) % 8), (1, pl.ds(0, 4), (d + 7) % 8)):
            for i, sub in enumerate((h, other)):
                copy = send(
                    ST.at[part], FR.at[st, h, side], ssF.at[st, i, side], rsF.at[st, h, side],
                    {"dom": peer, "sub": sub},
                )
                copy.start()
                dom_copies.append(copy)

        out = dot(ST[...].reshape(128, 128), WZ[...])
        scale = MODES[1 + h]
        r = MODES[0]
        for g in range(8):
            for t in range(4):
                for x2 in range(2):
                    row = (2 * g + x2) * 8
                    S2[8 * g + 2 * t + x2] = out[row : row + 8, t * 128 : t * 128 + 128] * scale

        p = zero8
        for i in range(64):
            p = p * r + jnp.where(low, S2[i], S2[63 - i])
            PP[i] = p
            if i == 47:
                MV[st, h, d, 0] = p
        MV[st, h, d, 1] = p
        mine = MV.at[st, h, d]
        for k in range(8):
            for i, sub in enumerate((h, other)):
                if k + i > 0:
                    copy = send(
                        mine, mine, ssM.at[st, i, k], rsM.at[st, h, k],
                        {"dom": (d + k) % 8, "sub": sub},
                    )
                    copy.start()
                    dom_copies.append(copy)

        def place(x, value):
            row = (2 * (x // 8) + x % 2) * 8
            t = (x % 8) // 2
            QB[row : row + 8, t * 128 : t * 128 + 128] = value

        def planes(q, put):
            out = dot(QB[...], WI[q])
            halo = zero8
            for g in range(8):
                for x2 in range(2):
                    j = 2 * g + x2
                    put(j, out[j * 8 : j * 8 + 8, :128])
                    part = out[j * 8 : j * 8 + 8, 128:]
                    halo = jnp.where(slot == x2 * 8 + g, part, halo)
            put(16, halo)

        for x in range(64):
            place(x, jnp.where(low, PP[x] - S2[x], PP[63 - x]))

        def to_other(j, value):
            OB[j] = value

        planes(other, to_other)
        copy_4 = send(OB, R4.at[st], ss4.at[st], rs4.at[st], {"sub": other})
        copy_4.start()

        def arrived(sub, index, sems, where):
            return send(where, where, sems.at[st, sub, index], sems.at[st, sub, index], {"sub": other})

        for side in range(2):
            for sub in range(2):
                arrived(sub, side, rsF, FR.at[st, sub, side]).wait_recv()
        out = dot(FR[st].reshape(128, 128), WZ[...])
        for side in range(2):
            for j in range(4):
                for t in range(4):
                    row = (side * 4 + j) * 8
                    span = slice(t * 128, t * 128 + 128)
                    value = out[row : row + 8, span] * MODES[1]
                    value = value + out[row + 64 : row + 72, span] * MODES[2]
                    S3[side * 16 + 8 * (j // 2) + 2 * t + j % 2] = value
        p = zero8
        for i in range(64):
            p = p * r
            if i < 16:
                p = p + jnp.where(low, S3[i], S3[31 - i])
            if i >= 48:
                p = p + jnp.where(low, S3[i - 32], S3[63 - i])
            P2[i] = PP[i] + p

        for k in range(8):
            for i, sub in enumerate((h, other)):
                if k + i > 0:
                    arrived(sub, k, rsM, MV.at[st, sub, (d + 8 - k) % 8]).wait_recv()

        def moment(k, which):
            left, right = (d + 16 - k) % 8, (d + k) % 8
            return jnp.where(
                low,
                MV[st, 0, left, which] + MV[st, 1, left, which],
                MV[st, 0, right, which] + MV[st, 1, right, which],
            )

        incoming = r * moment(1, 0)
        for k in range(2, 10):
            incoming = incoming + MODES[1 + k] * moment(k, 1)
        for x in range(64):
            source = S2[x]
            if x < 16:
                source = source + S3[x]
            if x >= 48:
                source = source + S3[x - 32]
            forth = P2[x] + PW[x] * incoming
            back = P2[63 - x] + PW[63 - x] * incoming
            place(x, jnp.where(low, forth - source, back))
        copy_4.wait_recv()

        def to_band(j, value):
            AG[st, b, j] = value + R4[st, j]

        planes(h, to_band)
        parts = (pl.ds(0, 8), pl.ds(8, 9))

        gather, forward = [], []

        def pass_on(index, k, half):
            block = AG.at[st, index, parts[half]]
            copy = send(block, block, ssH.at[st, k, half], rsH.at[st, k, half], {"band": mate})
            copy.start()
            forward.append((half, copy))

        for half, part in enumerate(parts):
            block = AG.at[st, b, part]
            for k in (2, 1, 3):
                copy = send(
                    block, block, ssG.at[st, k - 1, half], rsG.at[st, k - 1, half], {"band": zpeer(k)}
                )
                copy.start()
                gather.append((k, half, copy))
            pass_on(b, 0, half)
        for half in range(2):
            for k in (1, 3, 2):
                for kk, hh, copy in gather:
                    if (kk, hh) == (k, half):
                        copy.wait_recv()
                pass_on(zpeer(4 - k), k, half)
        for g in range(8):
            if g % 4 == 0:
                for half, copy in forward:
                    if half == g // 4:
                        copy.wait_recv()
            parts = [AG[st, :, 2 * g + x2].reshape(64, 128) for x2 in range(2)]
            cols = jnp.concatenate(parts, 0).T
            out = dot(cols, WY[...])
            for t in range(4):
                tile = 4 * g + t
                value = out[t * 32 : t * 32 + 32]
                VB[:, lanes(tile)] = value
                half = jnp.exp(-0.5 * TIME * (value + EXT[:, lanes(tile)]))
                HALF[:, lanes(tile)] = half
                HT[:, lanes(tile)] = 0.5 * TIME * half

        @pl.when(st == 0)
        def _():
            ext_copy.wait()

        edge_copy.wait_recv()
        rims = AG[st, :, 16].reshape(64, 128)
        out = dot(jnp.concatenate([rims, rims], 0).T, WH[...])
        low16 = lane16 < 64
        for t in range(4):
            value = jnp.where(low16, out[t * 32 : t * 32 + 16], out[t * 32 + 16 : t * 32 + 32])
            for g in range(8):
                tile = 4 * g + t
                for q in range(2):
                    HH[q, tile : tile + 1, :] = value[2 * g + q : 2 * g + q + 1]
        for q in range(2):
            half = jnp.exp(-0.5 * TIME * (HH[q] + EXTR[q]))
            for o in range(8):
                SH[q, o] = ER[st, q, o] * half * INV[o, 0:1, :]

        def advance(o, carry):
            inv = INV[o, 0:1, :]
            for c in range(4):
                rows = []
                for tile in range(8 * c, 8 * c + 8):
                    here = U[0, o, :, lanes(tile)] * HALF[:, lanes(tile)] * inv
                    SC[tile, 8:40] = here
                    SC[tile, 7:8] = SH[0, o, tile : tile + 1, :]
                    SC[tile, 40:41] = SH[1, o, tile : tile + 1, :]
                    coarse = here.astype(jnp.bfloat16)
                    fine = (here - coarse.astype(F32)).astype(jnp.bfloat16)
                    rows.append(jnp.concatenate([coarse, fine], 1))
                near = jnp.dot(jnp.concatenate(rows, 0), WS[...], preferred_element_type=F32)
                MX[8 * c : 8 * c + 8] = near.reshape(8, 32, 256)
            squares = zero8
            for tile in range(32):
                for i in range(4):
                    span = slice(8 * i, 8 * i + 8)
                    before = MX[tile - 1, span, 128:] if tile > 0 else zero8
                    after = MX[tile + 1, span, 128:] if tile < 31 else zero8
                    around = MX[tile, span, :128] + jnp.where(low, before, after)
                    around = around + SC[tile, 7 + 8 * i : 15 + 8 * i]
                    around = around + SC[tile, 9 + 8 * i : 17 + 8 * i]
                    value = around * HT[span, lanes(tile)]
                    U[0, o, span, lanes(tile)] = value
                    squares = squares + value * value
                    if i == 3:
                        EDGES[st + 1, 0, o, tile : tile + 1, :] = value[7:8]
                    if i == 0:
                        EDGES[st + 1, 1, o, tile : tile + 1, :] = value[0:1]
            NBO[o] = squares
            return carry

        lax.fori_loop(0, 8, advance, 0)

        for o in range(8):
            NB[st, o : o + 1, :] = jnp.sum(NBO[o], axis=0, keepdims=True)
        norm_copy = send(NB.at[st], NR.at[st], ssN.at[st], rsN.at[st], {"sub": other})
        norm_copy.start()

        @pl.when(st < STEPS - 1)
        def _():
            edges_of(st + 1).start()

        for copy in copies_a + copies_b + dom_copies + [copy_4]:
            copy.wait_send()
        for entry in gather + forward:
            entry[-1].wait_send()
        edge_copy.wait_send()
        norm_copy.wait()
        norms = jnp.sum(NB[st] + NR[st], axis=1, keepdims=True)
        inv = jnp.broadcast_to(1.0 / jnp.sqrt(norms / CELLS + EPS), (8, 128))
        for o in range(8):
            INV[o] = jnp.broadcast_to(inv[o : o + 1], (8, 128))
        W8[...] = OCC8[...] * inv * inv

        @pl.when(st < STEPS - 1)
        def _():
            density(st + 1, False)

        return carry

    lax.fori_loop(0, STEPS, step, 0)


def scale_out(U, VB, INV, out_hbm, pot_hbm, buffer, sems):
    copies = [pltpu.make_async_copy(VB, pot_hbm.at[0], sems.at[8])]
    copies[0].start()
    for o in range(8):
        for tile in range(32):
            lanes = pl.ds(tile * 128, 128)
            buffer[o, :, lanes] = U[0, o, :, lanes] * INV[o, 0:1, :]
        copy = pltpu.make_async_copy(buffer.at[o], out_hbm.at[0, o], sems.at[o])
        copy.start()
        copies.append(copy)
    for copy in copies:
        copy.wait()


def body(orbitals, occupations, ext_potential, core_range):
    operands = [orbitals, occupations, ext_potential, core_range]
    operands += [jnp.asarray(c) for c in tables()]
    hbm = pl.BlockSpec(memory_space=pltpu.HBM)
    smem = pl.BlockSpec(memory_space=pltpu.SMEM)
    vmem = pl.BlockSpec(memory_space=pltpu.VMEM)
    V = lambda *s: pltpu.VMEM(s, F32)
    D = lambda *s: pltpu.SemaphoreType.DMA(s)
    state, pot, inv = pl.pallas_call(
        kernel,
        out_shape=(
            pltpu.VMEM(orbitals.shape, F32),
            pltpu.VMEM(ext_potential.shape[1:], F32),
            pltpu.VMEM((8, 8, 128), F32),
        ),
        in_specs=[hbm, smem, hbm, smem] + [hbm] * 6,
        out_specs=(vmem, vmem, vmem),
        scratch_shapes=[
            V(32, 4096), V(32, 4096), V(32, 4096),
            V(128, 128), V(128, 128), V(128, 512), V(2, 512, 256), V(11, 8, 128),
            pltpu.VMEM((256, 256), jnp.bfloat16),
            V(8, 128), V(8, 128), V(32, 48, 128), V(32, 32, 256),
            V(2, 4, 16, 8, 128), V(3, 4, 16, 8, 128), V(4, 16, 8, 128), V(3, 3, 16, 8, 128),
            V(64, 8, 128), V(32, 8, 128), V(16, 8, 128), V(64, 8, 128), V(64, 8, 128), V(64, 8, 128),
            V(3, 2, 2, 4, 8, 128), V(3, 2, 8, 2, 8, 128), V(128, 512),
            V(17, 8, 128), V(3, 17, 8, 128), V(3, 8, 17, 8, 128),
            V(4, 2, 8, 32, 128), V(3, 2, 8, 32, 128), V(2, 32, 128), V(2, 32, 128), V(2, 32, 128),
            V(2, 8, 32, 128), V(8, 8, 128), V(3, 8, 128), V(3, 8, 128),
            D(2, 8), D(7), D(3, 2), D(3, 2), D(3, 3, 2), D(3, 3, 2), D(3, 2, 2), D(3, 2, 2), D(3, 2, 8), D(3, 2, 8),
            D(3), D(3), D(3, 3, 2), D(3, 3, 2), D(3, 4, 2), D(3, 4, 2),
            D(3), D(3), D(1), D(1), D(3), D(3),
        ],
        compiler_params=pltpu.CompilerParams(
            collective_id=0, has_side_effects=True, vmem_limit_bytes=59 * 1024 * 1024
        ),
        name="steps",
    )(
        *[
            v if i in (1, 3) else pltpu.with_memory_space_constraint(v, pltpu.HBM)
            for i, v in enumerate(operands)
        ]
    )
    return pl.pallas_call(
        scale_out,
        out_shape=(
            jax.ShapeDtypeStruct(orbitals.shape, F32),
            jax.ShapeDtypeStruct(ext_potential.shape, F32),
        ),
        in_specs=[vmem] * 3,
        out_specs=(hbm, hbm),
        scratch_shapes=[V(8, 32, 4096), D(9)],
        compiler_params=pltpu.CompilerParams(vmem_limit_bytes=8 * 1024 * 1024),
        name="scale_out",
    )(state, pot, inv)


def solution(mesh):
    return jax.shard_map(
        body,
        mesh=mesh,
        in_specs=(
            P("dom", "band", "sub", None),
            P("dom", "band"),
            P("dom", "sub", None),
            P("dom", None),
        ),
        out_specs=(P("dom", "band", "sub", None), P("dom", "sub", None)),
        check_vma=False,
    )
```

```python
import functools

import jax
import jax.numpy as jnp
import numpy as np
from jax import lax
from jax.experimental import pallas as pl
from jax.experimental.pallas import tpu as pltpu
from jax.sharding import PartitionSpec as P

EDGE = 64
MARGIN = 8
BLOCK = 4
STEPS = 3
CORE = 48
GX = 384
N_DOM = 8
N_BAND = 8
TIME = 0.2
SCREEN = 0.02
EPS = 1e-06
CELLS = float(EDGE**3)
F32 = jnp.float32
HIGH = lax.Precision.HIGH
MESH = pl.DeviceIdType.MESH


def cas(rows, cols, n):
    angle = 2.0 * np.pi / n * ((rows[:, None] * cols[None, :]) % n)
    return np.cos(angle) + np.sin(angle)


def halves(v):
    v = np.asarray(v, np.float32)
    coarse = v.astype(jnp.bfloat16)
    return np.stack([coarse, (v - coarse.astype(np.float32)).astype(jnp.bfloat16)])


def tables():
    ids = np.arange(EDGE)
    full = cas(ids, ids, EDGE)
    w_y = np.kron(np.eye(2), full)
    w_h = np.concatenate([np.concatenate([full, full], 1), np.zeros((64, 128))], 0)
    w_z = np.kron(np.eye(4), np.concatenate([full[:32], full[:32]], 1))
    both = np.concatenate([full, full], 0)
    halo0 = np.tile(both[:, [63, 32]], (1, 16))
    halo1 = np.tile(both[:, [31, 0]], (1, 16))
    w_i = [np.kron(np.eye(4), v) for v in (both[:, :32], halo0, both[:, 32:], halo1)]
    w_i = np.stack([np.concatenate(w_i[:2], 1), np.concatenate(w_i[2:], 1)])
    lam = 2.0 - 2.0 * np.cos(2.0 * np.pi / EDGE * ids)
    a = lam[:, None] + lam[None, :] + SCREEN
    r = 1.0 / (1.0 + a / 2 + np.sqrt(a + a * a / 4))
    scale = 1.0 / (1.0 / r - r) / (EDGE * EDGE)
    sign = np.where(ids % 2 == 1, -1.0, 1.0)[None, :]
    rows = [r, scale, scale * sign]
    for k in range(2, 10):
        rows.append(r ** (CORE * k - 63) / (1.0 - r**GX))
    modes = np.stack(rows)
    modes = np.concatenate([modes, modes], 2).reshape(11, N_BAND, 8, 128).transpose(1, 0, 2, 3)
    swap = np.kron(1.0 - np.eye(2), np.eye(64))
    ring = np.roll(np.eye(64), 1, 0) + np.roll(np.eye(64), -1, 0)
    ring = ring + (1.0 / (0.5 * TIME) - 6.0) * np.eye(64)
    stencil = np.concatenate([np.kron(np.eye(2), ring) + swap, swap], 1)
    stencil = np.concatenate([stencil, stencil], 0)
    out = [np.asarray(v, np.float32) for v in (w_y, w_h)] + [halves(w_z), halves(w_i)]
    out.append(np.asarray(modes, np.float32))
    return out + [np.asarray(stencil, jnp.bfloat16)]


def dot(a, b, dims=((1,), (0,))):
    return lax.dot_general(a, b, (dims, ((), ())), precision=HIGH, preferred_element_type=F32)


def dot_split(a, coarse_b, fine_b):
    coarse = a.astype(jnp.bfloat16)
    fine = (a - coarse.astype(F32)).astype(jnp.bfloat16)
    out = jnp.dot(coarse, coarse_b, preferred_element_type=F32)
    out = out + jnp.dot(fine, coarse_b, preferred_element_type=F32)
    return out + jnp.dot(coarse, fine_b, preferred_element_type=F32)


def kernel(
    orb_hbm, occ, ext_hbm, core, wy_hbm, wh_hbm, wz_hbm, wi_hbm, modes_hbm, st_hbm,
    U, VB, INV,
    HALF, HT, EXT, WY, WH, WZ, WI, MODES, WS, OCC8, W8, SC, MX,
    SB, RA, S1, RB, S2, S3, ST, PP, P2, PW, FR, MV, QB, OB, R4, AG, EDGES, ER, EXTE, EXTR, HH, SH, NBO, NB, NR,
    l_u, l_c, ssA, rsA, ssB, rsB, ssF, rsF, ssM, rsM, ss4, rs4, ssG, rsG, ssH, rsH, ssE, rsE,
    ssX, rsX, ssN, rsN,
):
    d = lax.axis_index("dom")
    b = lax.axis_index("band")
    h = lax.axis_index("sub")
    zi = b // 2
    co = b % 2
    mate = zi * 2 + (1 - co)
    other = 1 - h

    def zpeer(k):
        return ((zi + k) % 4) * 2 + co

    loads = [
        pltpu.make_async_copy(
            orb_hbm.at[0, o, :, pl.ds(2048 * half, 2048)],
            U.at[0, o, :, pl.ds(2048 * half, 2048)],
            l_u.at[half, o],
        )
        for half in range(2)
        for o in range(8)
    ]
    consts = [
        pltpu.make_async_copy(src, dst, l_c.at[i])
        for i, (src, dst) in enumerate(
            (
                (wy_hbm, WY),
                (ext_hbm.at[0], EXT),
                (wh_hbm, WH),
                (wz_hbm, WZ),
                (wi_hbm, WI),
                (modes_hbm.at[b], MODES),
                (st_hbm, WS),
            )
        )
    ]
    for c in consts[:1] + loads:
        c.start()

    barrier = pltpu.get_barrier_semaphore()

    def greet(dev):
        pl.semaphore_signal(barrier, inc=1, device_id=dev, device_id_type=MESH)

    greet({"band": mate})
    for k in range(1, 4):
        greet({"band": zpeer(k)})
    greet({"sub": other})
    for k in range(1, 8):
        for sub in (h, other):
            greet({"dom": (d + k) % 8, "sub": sub})

    def send(src, dst, ss, rs, dev):
        return pltpu.make_async_remote_copy(
            src_ref=src, dst_ref=dst, send_sem=ss, recv_sem=rs, device_id=dev, device_id_type=MESH
        )

    lane = lax.broadcasted_iota(jnp.int32, (8, 128), 1)
    low = lane < 64
    lane16 = lax.broadcasted_iota(jnp.int32, (16, 128), 1)
    lane32 = lax.broadcasted_iota(jnp.int32, (32, 128), 1)
    slot = (lane % 32) // 2
    zero8 = jnp.zeros((8, 128), F32)

    for o in range(8):
        OCC8[o : o + 1, :] = jnp.full((1, 128), occ[0, o], F32)
    W8[...] = OCC8[...]
    INV[...] = jnp.ones((8, 8, 128), F32)

    def lanes(tile):
        return pl.ds(tile * 128, 128)

    low_x = core[0, 0] * BLOCK
    high_x = core[0, 1] * BLOCK

    def to_mate(st, half):
        part = pl.ds(8 * half, 8)
        return send(
            SB.at[1 - co, :, part], RA.at[st, :, part], ssA.at[st, half], rsA.at[st, half],
            {"band": mate},
        )

    def edges_of(st):
        return send(EDGES.at[st], ER.at[st], ssE.at[st], rsE.at[st], {"sub": other})

    def weighted(tile, start):
        acc = jnp.zeros((32, 128), F32)
        for o in range(start, start + 4):
            value = U[0, o, :, lanes(tile)]
            acc = acc + value * value * W8[o : o + 1, :]
        return acc

    def density(st, first):
        for g in range(8):
            if first and g % 4 == 0:
                for c in loads[2 * g : 2 * g + 8]:
                    c.wait()
            tiles = []
            for t in range(4):
                tile = 4 * g + t
                acc = weighted(tile, 0) if first else SC[tile, 8:40]
                acc = acc + weighted(tile, 4)
                x = 2 * tile + lane32 // 64
                tiles.append(jnp.where((x >= low_x) & (x < high_x), acc, 0.0))
            rho = jnp.concatenate(tiles, 0)
            out = dot(WY[...], rho, ((1,), (1,)))
            for x2 in range(2):
                for c in range(2):
                    for z in range(4):
                        row = x2 * 64 + (2 * z + c) * 8
                        SB[c, z, 2 * g + x2] = out[row : row + 8]
            if g == 3 and first:
                pl.semaphore_wait(barrier, 19)
            if g % 4 == 3:
                to_mate(st, g // 4).start()

    consts[0].wait()
    for c in consts[1:]:
        c.start()
    density(0, True)
    for c in consts[1:]:
        c.wait()

    for tile in range(32):
        EXTE[0, tile : tile + 1, :] = EXT[31:32, lanes(tile)]
        EXTE[1, tile : tile + 1, :] = EXT[0:1, lanes(tile)]

    def first_edges(o, carry):
        for tile in range(32):
            EDGES[0, 0, o, tile : tile + 1, :] = U[0, o, 31:32, lanes(tile)]
            EDGES[0, 1, o, tile : tile + 1, :] = U[0, o, 0:1, lanes(tile)]
        return carry

    lax.fori_loop(0, 8, first_edges, 0)
    ext_copy = send(EXTE, EXTR, ssX.at[0], rsX.at[0], {"sub": other})
    ext_copy.start()
    edges_of(0).start()

    r = MODES[0]
    power = jnp.ones((8, 128), F32)
    for i in range(64):
        PW[i] = power
        power = power * r

    def step(st, carry):
        edge_copy = edges_of(st)

        copies_a = [to_mate(st, half) for half in range(2)]
        copies_b = []
        for half in range(2):
            part = pl.ds(8 * half, 8)
            copies_a[half].wait_recv()
            for k in (2, 1, 3):
                z = (zi + k) % 4
                S1[k, part] = SB[co, z, part] + RA[st, z, part]
                copy = send(
                    S1.at[k, part], RB.at[st, k - 1, part], ssB.at[st, k - 1, half],
                    rsB.at[st, k - 1, half], {"band": zpeer(k)},
                )
                copy.start()
                copies_b.append(copy)
            S1[0, part] = SB[co, zi, part] + RA[st, zi, part]
        for copy in copies_b:
            copy.wait_recv()
        ST[...] = S1[0] + RB[st, 0] + RB[st, 1] + RB[st, 2]

        dom_copies = []
        for side, part, peer in ((0, pl.ds(12, 4), (d + 1) % 8), (1, pl.ds(0, 4), (d + 7) % 8)):
            for i, sub in enumerate((h, other)):
                copy = send(
                    ST.at[part], FR.at[st, h, side], ssF.at[st, i, side], rsF.at[st, h, side],
                    {"dom": peer, "sub": sub},
                )
                copy.start()
                dom_copies.append(copy)

        out = dot_split(ST[...].reshape(128, 128), WZ[0], WZ[1])
        scale = MODES[1 + h]
        r = MODES[0]
        for g in range(8):
            for t in range(4):
                for x2 in range(2):
                    row = (2 * g + x2) * 8
                    S2[8 * g + 2 * t + x2] = out[row : row + 8, t * 128 : t * 128 + 128] * scale

        p = zero8
        for i in range(64):
            p = p * r + jnp.where(low, S2[i], S2[63 - i])
            PP[i] = p
            if i == 47:
                MV[st, h, d, 0] = p
        MV[st, h, d, 1] = p
        mine = MV.at[st, h, d]
        for k in range(8):
            for i, sub in enumerate((h, other)):
                if k + i > 0:
                    copy = send(
                        mine, mine, ssM.at[st, i, k], rsM.at[st, h, k],
                        {"dom": (d + k) % 8, "sub": sub},
                    )
                    copy.start()
                    dom_copies.append(copy)

        def place(x, value):
            row = (2 * (x // 8) + x % 2) * 8
            t = (x % 8) // 2
            QB[row : row + 8, t * 128 : t * 128 + 128] = value

        def planes(q, put):
            out = dot_split(QB[...], WI[0, q], WI[1, q])
            halo = zero8
            for g in range(8):
                for x2 in range(2):
                    j = 2 * g + x2
                    put(j, out[j * 8 : j * 8 + 8, :128])
                    part = out[j * 8 : j * 8 + 8, 128:]
                    halo = jnp.where(slot == x2 * 8 + g, part, halo)
            put(16, halo)

        for x in range(64):
            place(x, jnp.where(low, PP[x] - S2[x], PP[63 - x]))

        def to_other(j, value):
            OB[j] = value

        planes(other, to_other)
        copy_4 = send(OB, R4.at[st], ss4.at[st], rs4.at[st], {"sub": other})
        copy_4.start()

        def arrived(sub, index, sems, where):
            return send(where, where, sems.at[st, sub, index], sems.at[st, sub, index], {"sub": other})

        for side in range(2):
            for sub in range(2):
                arrived(sub, side, rsF, FR.at[st, sub, side]).wait_recv()
        out = dot_split(FR[st].reshape(128, 128), WZ[0], WZ[1])
        for side in range(2):
            for j in range(4):
                for t in range(4):
                    row = (side * 4 + j) * 8
                    span = slice(t * 128, t * 128 + 128)
                    value = out[row : row + 8, span] * MODES[1]
                    value = value + out[row + 64 : row + 72, span] * MODES[2]
                    S3[side * 16 + 8 * (j // 2) + 2 * t + j % 2] = value
        p = zero8
        for i in range(64):
            p = p * r
            if i < 16:
                p = p + jnp.where(low, S3[i], S3[31 - i])
            if i >= 48:
                p = p + jnp.where(low, S3[i - 32], S3[63 - i])
            P2[i] = PP[i] + p

        for k in range(8):
            for i, sub in enumerate((h, other)):
                if k + i > 0:
                    arrived(sub, k, rsM, MV.at[st, sub, (d + 8 - k) % 8]).wait_recv()

        def moment(k, which):
            left, right = (d + 16 - k) % 8, (d + k) % 8
            return jnp.where(
                low,
                MV[st, 0, left, which] + MV[st, 1, left, which],
                MV[st, 0, right, which] + MV[st, 1, right, which],
            )

        incoming = r * moment(1, 0)
        for k in range(2, 10):
            incoming = incoming + MODES[1 + k] * moment(k, 1)
        for x in range(64):
            source = S2[x]
            if x < 16:
                source = source + S3[x]
            if x >= 48:
                source = source + S3[x - 32]
            forth = P2[x] + PW[x] * incoming
            back = P2[63 - x] + PW[63 - x] * incoming
            place(x, jnp.where(low, forth - source, back))
        copy_4.wait_recv()

        def to_band(j, value):
            AG[st, b, j] = value + R4[st, j]

        planes(h, to_band)
        parts = (pl.ds(0, 8), pl.ds(8, 9))

        gather, forward = [], []

        def pass_on(index, k, half):
            block = AG.at[st, index, parts[half]]
            copy = send(block, block, ssH.at[st, k, half], rsH.at[st, k, half], {"band": mate})
            copy.start()
            forward.append((half, copy))

        for half, part in enumerate(parts):
            block = AG.at[st, b, part]
            for k in (2, 1, 3):
                copy = send(
                    block, block, ssG.at[st, k - 1, half], rsG.at[st, k - 1, half], {"band": zpeer(k)}
                )
                copy.start()
                gather.append((k, half, copy))
            pass_on(b, 0, half)
        for half in range(2):
            for k in (1, 3, 2):
                for kk, hh, copy in gather:
                    if (kk, hh) == (k, half):
                        copy.wait_recv()
                pass_on(zpeer(4 - k), k, half)
        for g in range(8):
            if g % 4 == 0:
                for half, copy in forward:
                    if half == g // 4:
                        copy.wait_recv()
            parts = [AG[st, :, 2 * g + x2].reshape(64, 128) for x2 in range(2)]
            cols = jnp.concatenate(parts, 0).T
            out = dot(cols, WY[...])
            for t in range(4):
                tile = 4 * g + t
                value = out[t * 32 : t * 32 + 32]
                VB[:, lanes(tile)] = value
                half = jnp.exp(-0.5 * TIME * (value + EXT[:, lanes(tile)]))
                HALF[:, lanes(tile)] = half
                HT[:, lanes(tile)] = 0.5 * TIME * half

        @pl.when(st == 0)
        def _():
            ext_copy.wait()

        edge_copy.wait_recv()
        rims = AG[st, :, 16].reshape(64, 128)
        out = dot(jnp.concatenate([rims, rims], 0).T, WH[...])
        low16 = lane16 < 64
        for t in range(4):
            value = jnp.where(low16, out[t * 32 : t * 32 + 16], out[t * 32 + 16 : t * 32 + 32])
            for g in range(8):
                tile = 4 * g + t
                for q in range(2):
                    HH[q, tile : tile + 1, :] = value[2 * g + q : 2 * g + q + 1]
        for q in range(2):
            half = jnp.exp(-0.5 * TIME * (HH[q] + EXTR[q]))
            for o in range(8):
                SH[q, o] = ER[st, q, o] * half * INV[o, 0:1, :]

        def advance(o, carry):
            inv = INV[o, 0:1, :]
            for c in range(4):
                rows = []
                for tile in range(8 * c, 8 * c + 8):
                    here = U[0, o, :, lanes(tile)] * HALF[:, lanes(tile)] * inv
                    SC[tile, 8:40] = here
                    SC[tile, 7:8] = SH[0, o, tile : tile + 1, :]
                    SC[tile, 40:41] = SH[1, o, tile : tile + 1, :]
                    coarse = here.astype(jnp.bfloat16)
                    fine = (here - coarse.astype(F32)).astype(jnp.bfloat16)
                    rows.append(jnp.concatenate([coarse, fine], 1))
                near = jnp.dot(jnp.concatenate(rows, 0), WS[...], preferred_element_type=F32)
                MX[8 * c : 8 * c + 8] = near.reshape(8, 32, 256)
            squares = zero8
            for tile in range(32):
                for i in range(4):
                    span = slice(8 * i, 8 * i + 8)
                    before = MX[tile - 1, span, 128:] if tile > 0 else zero8
                    after = MX[tile + 1, span, 128:] if tile < 31 else zero8
                    around = MX[tile, span, :128] + jnp.where(low, before, after)
                    around = around + SC[tile, 7 + 8 * i : 15 + 8 * i]
                    around = around + SC[tile, 9 + 8 * i : 17 + 8 * i]
                    value = around * HT[span, lanes(tile)]
                    U[0, o, span, lanes(tile)] = value
                    squares = squares + value * value
                    if i == 3:
                        EDGES[st + 1, 0, o, tile : tile + 1, :] = value[7:8]
                    if i == 0:
                        EDGES[st + 1, 1, o, tile : tile + 1, :] = value[0:1]
            NBO[o] = squares
            return carry

        norm_copies = []
        for half in range(2):
            lax.fori_loop(4 * half, 4 * half + 4, advance, 0)
            for i in range(8):
                NB[st, half, i : i + 1, :] = jnp.sum(NBO[4 * half + i % 4], axis=0, keepdims=True)
            copy = send(NB.at[st, half], NR.at[st, half], ssN.at[st, half], rsN.at[st, half], {"sub": other})
            copy.start()
            norm_copies.append(copy)

        @pl.when(st < STEPS - 1)
        def _():
            edges_of(st + 1).start()

        for copy in copies_a + copies_b + dom_copies + [copy_4]:
            copy.wait_send()
        for entry in gather + forward:
            entry[-1].wait_send()
        edge_copy.wait_send()

        def normalize(half):
            norm_copies[half].wait()
            norms = jnp.sum(NB[st, half] + NR[st, half], axis=1, keepdims=True)
            inv = jnp.broadcast_to(1.0 / jnp.sqrt(norms / CELLS + EPS), (8, 128))[:4]
            for i in range(4):
                INV[4 * half + i] = jnp.broadcast_to(inv[i : i + 1], (8, 128))
            span = slice(4 * half, 4 * half + 4)
            W8[span, :] = OCC8[span, :] * inv * inv

        normalize(0)

        @pl.when(st < STEPS - 1)
        def _():
            for tile in range(32):
                SC[tile, 8:40] = weighted(tile, 0)

        normalize(1)

        @pl.when(st < STEPS - 1)
        def _():
            density(st + 1, False)

        return carry

    lax.fori_loop(0, STEPS, step, 0)


def scale_out(U, VB, INV, out_hbm, pot_hbm, buffer, sems):
    copies = [pltpu.make_async_copy(VB, pot_hbm.at[0], sems.at[8])]
    copies[0].start()
    for o in range(8):
        for tile in range(32):
            lanes = pl.ds(tile * 128, 128)
            buffer[o, :, lanes] = U[0, o, :, lanes] * INV[o, 0:1, :]
        copy = pltpu.make_async_copy(buffer.at[o], out_hbm.at[0, o], sems.at[o])
        copy.start()
        copies.append(copy)
    for copy in copies:
        copy.wait()


def body(orbitals, occupations, ext_potential, core_range):
    operands = [orbitals, occupations, ext_potential, core_range]
    operands += [jnp.asarray(c) for c in tables()]
    hbm = pl.BlockSpec(memory_space=pltpu.HBM)
    smem = pl.BlockSpec(memory_space=pltpu.SMEM)
    vmem = pl.BlockSpec(memory_space=pltpu.VMEM)
    V = lambda *s: pltpu.VMEM(s, F32)
    D = lambda *s: pltpu.SemaphoreType.DMA(s)
    state, pot, inv = pl.pallas_call(
        kernel,
        out_shape=(
            pltpu.VMEM(orbitals.shape, F32),
            pltpu.VMEM(ext_potential.shape[1:], F32),
            pltpu.VMEM((8, 8, 128), F32),
        ),
        in_specs=[hbm, smem, hbm, smem] + [hbm] * 6,
        out_specs=(vmem, vmem, vmem),
        scratch_shapes=[
            V(32, 4096), V(32, 4096), V(32, 4096),
            V(128, 128), V(128, 128), pltpu.VMEM((2, 128, 512), jnp.bfloat16), pltpu.VMEM((2, 2, 512, 256), jnp.bfloat16), V(11, 8, 128),
            pltpu.VMEM((256, 256), jnp.bfloat16),
            V(8, 128), V(8, 128), V(32, 48, 128), V(32, 32, 256),
            V(2, 4, 16, 8, 128), V(3, 4, 16, 8, 128), V(4, 16, 8, 128), V(3, 3, 16, 8, 128),
            V(64, 8, 128), V(32, 8, 128), V(16, 8, 128), V(64, 8, 128), V(64, 8, 128), V(64, 8, 128),
            V(3, 2, 2, 4, 8, 128), V(3, 2, 8, 2, 8, 128), V(128, 512),
            V(17, 8, 128), V(3, 17, 8, 128), V(3, 8, 17, 8, 128),
            V(4, 2, 8, 32, 128), V(3, 2, 8, 32, 128), V(2, 32, 128), V(2, 32, 128), V(2, 32, 128),
            V(2, 8, 32, 128), V(8, 8, 128), V(3, 2, 8, 128), V(3, 2, 8, 128),
            D(2, 8), D(7), D(3, 2), D(3, 2), D(3, 3, 2), D(3, 3, 2), D(3, 2, 2), D(3, 2, 2), D(3, 2, 8), D(3, 2, 8),
            D(3), D(3), D(3, 3, 2), D(3, 3, 2), D(3, 4, 2), D(3, 4, 2),
            D(3), D(3), D(1), D(1), D(3, 2), D(3, 2),
        ],
        compiler_params=pltpu.CompilerParams(
            collective_id=0, has_side_effects=True, vmem_limit_bytes=59 * 1024 * 1024
        ),
        name="steps",
    )(
        *[
            v if i in (1, 3) else pltpu.with_memory_space_constraint(v, pltpu.HBM)
            for i, v in enumerate(operands)
        ]
    )
    return pl.pallas_call(
        scale_out,
        out_shape=(
            jax.ShapeDtypeStruct(orbitals.shape, F32),
            jax.ShapeDtypeStruct(ext_potential.shape, F32),
        ),
        in_specs=[vmem] * 3,
        out_specs=(hbm, hbm),
        scratch_shapes=[V(8, 32, 4096), D(9)],
        compiler_params=pltpu.CompilerParams(vmem_limit_bytes=8 * 1024 * 1024),
        name="scale_out",
    )(state, pot, inv)


def solution(mesh):
    return jax.shard_map(
        body,
        mesh=mesh,
        in_specs=(
            P("dom", "band", "sub", None),
            P("dom", "band"),
            P("dom", "sub", None),
            P("dom", None),
        ),
        out_specs=(P("dom", "band", "sub", None), P("dom", "sub", None)),
        check_vma=False,
    )
```
